128 devices in a mesh: dp: 1, sp: 128 (over z, y, x, core).
Axes of the slice: x: 4, y: 4, z: 4, core: 2. Of those that a mesh axis runs over, the one named last changes fastest.
Arguments:
- patches: bfloat16 [2, 8192, 768], P('dp', 'sp')
- vis_mask: int32 [2, 8192], P('dp', 'sp')
- enc_pos: bfloat16 [8192, 1024], P(('dp', 'sp'))
- dec_pos: bfloat16 [8192, 512], P(('dp', 'sp'))
- w_pe: bfloat16 [768, 1024], replicated
- b_pe: bfloat16 [1024], replicated
- enc_qkv: bfloat16 [2, 1024, 3, 16, 64], replicated
- enc_proj: bfloat16 [2, 16, 64, 1024], replicated
- enc_up: bfloat16 [2, 1024, 4096], replicated
- enc_down: bfloat16 [2, 4096, 1024], replicated
- w_ed: bfloat16 [1024, 512], replicated
- mask_token: bfloat16 [512], replicated
- dec_qkv: bfloat16 [2, 512, 3, 16, 32], replicated
- dec_proj: bfloat16 [2, 16, 32, 512], replicated
- dec_up: bfloat16 [2, 512, 2048], replicated
- dec_down: bfloat16 [2, 2048, 512], replicated
- w_out: bfloat16 [512, 768], replicated
Outputs:
- output: float32 [2, 8192, 768], P('dp', 'sp')
All inputs are finite; a program needn't handle non-finite values.
Results may differ from the reference program's by a relative error of at most 0.0153618.
Values are sent between devices in bfloat16 or wider.
A program may use at most 1 GiB of HBM per device.

```python
import jax
import jax.numpy as jnp
from jax import lax

P = 768
D = 1024
ENC_HEADS = 16
DD = 512
DEC_HEADS = 16
TOK_DEV = 64
SP = 128
KEEP_DIV = 8
CLIPS = 2
LAYERS = 2

SEQ = TOK_DEV * SP
VIS_SHARD = TOK_DEV // KEEP_DIV
VIS_ALL = VIS_SHARD * SP
ENC_HD = D // ENC_HEADS
DEC_HD = DD // DEC_HEADS


def shard_ranks(key):
    return jax.random.permutation(key, TOK_DEV)


def draw_mask(key):
    half_shard = VIS_SHARD // 2
    key_shift, key_pick, key_perm = jax.random.split(key, 3)
    inner_shift = jax.random.randint(key_shift, (CLIPS, SP - 1), -half_shard, half_shard + 1)
    pick_at = jax.random.randint(key_pick, (CLIPS, 1), 1, SP - 2)
    shard_idx = jnp.arange(1, SP)[None, :]
    inner_shift = jnp.where(shard_idx == pick_at, half_shard, inner_shift)
    inner_shift = jnp.where(shard_idx == pick_at + 1, -half_shard, inner_shift)
    inner_shift = jnp.where(shard_idx == pick_at + 2, half_shard, inner_shift)
    edge_zero = jnp.zeros((CLIPS, 1), jnp.int32)
    shift_all = jnp.concatenate([edge_zero, inner_shift, edge_zero], axis=1)
    shard_counts = VIS_SHARD + shift_all[:, 1:] - shift_all[:, :-1]
    tok_ranks = jax.vmap(shard_ranks)(jax.random.split(key_perm, CLIPS * SP))
    tok_ranks = tok_ranks.reshape(CLIPS, SP, TOK_DEV)
    return (tok_ranks < shard_counts[:, :, None]).astype(jnp.int32).reshape(CLIPS, SEQ)


def draw_normal(key, shape, scale):
    return (scale * jax.random.normal(key, shape, jnp.float32)).astype(jnp.bfloat16)


def setup_inputs(seed: int = 0, part: int = 0) -> dict:
    key_shared, key_local = jax.random.split(jax.random.key(seed))
    part_keys = jax.random.split(jax.random.fold_in(key_local, part), 4)
    weight_keys = jax.random.split(key_shared, 13)
    return {
        'patches': draw_normal(part_keys[0], (CLIPS, SEQ, P), 1.0),
        'vis_mask': draw_mask(part_keys[1]),
        'enc_pos': draw_normal(part_keys[2], (SEQ, D), 0.5),
        'dec_pos': draw_normal(part_keys[3], (SEQ, DD), 0.5),
        'w_pe': draw_normal(weight_keys[0], (P, D), P ** -0.5),
        'b_pe': draw_normal(weight_keys[1], (D,), 0.5),
        'enc_qkv': draw_normal(weight_keys[2], (LAYERS, D, 3, ENC_HEADS, ENC_HD), 1.5 * D ** -0.5),
        'enc_proj': draw_normal(weight_keys[3], (LAYERS, ENC_HEADS, ENC_HD, D), D ** -0.5),
        'enc_up': draw_normal(weight_keys[4], (LAYERS, D, 4 * D), D ** -0.5),
        'enc_down': draw_normal(weight_keys[5], (LAYERS, 4 * D, D), (4 * D) ** -0.5),
        'w_ed': draw_normal(weight_keys[6], (D, DD), D ** -0.5),
        'mask_token': draw_normal(weight_keys[7], (DD,), 1.0),
        'dec_qkv': draw_normal(weight_keys[8], (LAYERS, DD, 3, DEC_HEADS, DEC_HD), 1.5 * DD ** -0.5),
        'dec_proj': draw_normal(weight_keys[9], (LAYERS, DEC_HEADS, DEC_HD, DD), DD ** -0.5),
        'dec_up': draw_normal(weight_keys[10], (LAYERS, DD, 4 * DD), DD ** -0.5),
        'dec_down': draw_normal(weight_keys[11], (LAYERS, 4 * DD, DD), (4 * DD) ** -0.5),
        'w_out': draw_normal(weight_keys[12], (DD, P), DD ** -0.5),
    }


def layer_norm(hidden):
    hid_f32 = hidden.astype(jnp.float32)
    centred = hid_f32 - jnp.mean(hid_f32, axis=-1, keepdims=True)
    row_var = jnp.mean(centred * centred, axis=-1, keepdims=True)
    return (centred * lax.rsqrt(row_var + 1e-6)).astype(jnp.bfloat16)


def attend(queries, key_rows, value_rows):
    q_rows, n_heads, head_dim = queries.shape
    keys_f32 = key_rows.astype(jnp.float32)
    values_f32 = value_rows.astype(jnp.float32)

    def one_block(q_block):
        scores = jnp.einsum('qhk,shk->hqs', q_block.astype(jnp.float32), keys_f32) * head_dim ** -0.5
        attn_probs = jax.nn.softmax(scores, axis=-1).astype(jnp.bfloat16)
        return jnp.einsum('hqs,shk->qhk', attn_probs.astype(jnp.float32), values_f32).astype(jnp.bfloat16)

    q_blocks = queries.reshape(SP, q_rows // SP, n_heads, head_dim)
    return lax.map(one_block, q_blocks).reshape(q_rows, n_heads, head_dim)


def block(hidden, w_qkv, w_proj, w_up, w_down):
    proj_qkv = jnp.einsum('nd,dshk->snhk', layer_norm(hidden).astype(jnp.float32), w_qkv.astype(jnp.float32)).astype(jnp.bfloat16)
    attended = attend(proj_qkv[0], proj_qkv[1], proj_qkv[2])
    att_out = jnp.einsum('nhk,hkd->nd', attended.astype(jnp.float32), w_proj.astype(jnp.float32))
    mid_state = (hidden.astype(jnp.float32) + att_out).astype(jnp.bfloat16)
    up_act = jax.nn.gelu(jnp.dot(layer_norm(mid_state), w_up, preferred_element_type=jnp.float32), approximate=False).astype(jnp.bfloat16)
    return (mid_state.astype(jnp.float32) + jnp.dot(up_act, w_down, preferred_element_type=jnp.float32)).astype(jnp.bfloat16)


def run_stack(hidden, w_qkv, w_proj, w_up, w_down):
    def body(carry, layer_w):
        return block(carry, layer_w[0], layer_w[1], layer_w[2], layer_w[3]), None

    final_state, unused = lax.scan(body, hidden, (w_qkv, w_proj, w_up, w_down))
    return final_state


def reference(patches, vis_mask, enc_pos, dec_pos, w_pe, b_pe, enc_qkv, enc_proj, enc_up, enc_down, w_ed, mask_token, dec_qkv, dec_proj, dec_up, dec_down, w_out):
    def one_clip(clip_in):
        clip_patches, visible = clip_in
        vis_idx = jnp.nonzero(visible, size=VIS_ALL)[0]
        embedded = (jnp.dot(clip_patches[vis_idx], w_pe, preferred_element_type=jnp.float32)
                    + b_pe.astype(jnp.float32) + enc_pos[vis_idx].astype(jnp.float32)).astype(jnp.bfloat16)
        encoded = run_stack(embedded, enc_qkv, enc_proj, enc_up, enc_down)
        z_vis = jnp.dot(layer_norm(encoded), w_ed, preferred_element_type=jnp.float32).astype(jnp.bfloat16)
        vis_rank = jnp.clip(jnp.cumsum(visible) - visible, 0, VIS_ALL - 1)
        dec_tok = jnp.where(visible[:, None] == 1, z_vis[vis_rank], mask_token[None, :])
        dec_in = (dec_tok.astype(jnp.float32) + dec_pos.astype(jnp.float32)).astype(jnp.bfloat16)
        decoded = run_stack(dec_in, dec_qkv, dec_proj, dec_up, dec_down)
        return jnp.dot(layer_norm(decoded), w_out, preferred_element_type=jnp.float32)

    return lax.map(one_clip, (patches, vis_mask))
```

```python
import functools

import jax
import jax.numpy as jnp
from jax import lax
from jax.experimental import pallas as pl
from jax.experimental.pallas import tpu as pltpu
from jax.sharding import PartitionSpec as P

KEEP_DIV = 8
LANES = 128
LOG2E = 1.4426950408889634
NEG = -3e38


def layer_norm(hidden):
    hid_f32 = hidden.astype(jnp.float32)
    centred = hid_f32 - jnp.mean(hid_f32, axis=-1, keepdims=True)
    row_var = jnp.mean(centred * centred, axis=-1, keepdims=True)
    return (centred * lax.rsqrt(row_var + 1e-6)).astype(jnp.bfloat16)


def lane_iota(shape):
    return lax.broadcasted_iota(jnp.int32, shape, len(shape) - 1)


def flash(q, kv_ref, n_keys, bk, scale, mask_ref=None):
    rows = q.shape[0]
    c = scale * LOG2E

    def body(step, carry):
        m, l, acc = carry
        start = pl.multiple_of(step * bk, bk)
        kv = kv_ref[pl.ds(start, bk), :]
        s = lax.dot_general(q, kv, (((1,), (1,)), ((), ())), preferred_element_type=jnp.float32)
        m_new = jnp.maximum(m, jnp.max(s, axis=1, keepdims=True))
        p = jnp.exp2(s * c - m_new * c)
        alpha = jnp.exp2((m - m_new) * c)
        l = l * alpha + jnp.sum(p, axis=1, keepdims=True)
        acc = acc * alpha + jnp.dot(p.astype(jnp.bfloat16), kv[:, :LANES], preferred_element_type=jnp.float32)
        return m_new, l, acc

    init = (jnp.full((rows, 1), NEG, jnp.float32), jnp.zeros((rows, 1), jnp.float32), jnp.zeros((rows, LANES), jnp.float32))
    return lax.fori_loop(0, n_keys // bk, body, init)


def wait_bytes(ref, sem):
    pltpu.make_async_copy(ref, ref, sem).wait()


def attention_kernel(n, rows_kv, decoder, scale, bq, bk, kvm_ref, qm_ref, om_ref, kv_s, q_s, o_s, kvx_s, kv_send, kv_recv, q_send, q_recv, o_send, o_recv):
    me = lax.axis_index('sp')
    groups = n // 4
    pair = me // 4

    barrier = pltpu.get_barrier_semaphore()

    def greet(i, _):
        pl.semaphore_signal(barrier, inc=1, device_id={'sp': lax.rem(me + i, n)}, device_id_type=pl.DeviceIdType.MESH)
        return 0

    lax.fori_loop(1, n, greet, 0)
    pl.semaphore_wait(barrier, n - 1)

    def send_q(k, _):
        to = lax.rem(me + 4 * k, n)
        pltpu.make_async_remote_copy(
            src_ref=qm_ref.at[to // 4], dst_ref=q_s.at[k], send_sem=q_send, recv_sem=q_recv,
            device_id={'sp': to}, device_id_type=pl.DeviceIdType.MESH).start()
        return 0

    def send_kv(i, _):
        to = lax.rem(me + i, n)
        pltpu.make_async_remote_copy(
            src_ref=kvm_ref.at[to // 4], dst_ref=kv_s.at[i], send_sem=kv_send, recv_sem=kv_recv,
            device_id={'sp': to}, device_id_type=pl.DeviceIdType.MESH).start()
        return 0

    lax.fori_loop(1, groups, send_q, 0)
    lax.fori_loop(1, n, send_kv, 0)
    q_s[0] = qm_ref[pair]
    kv_s[0] = kvm_ref[pair]

    wait_bytes(q_s.at[pl.ds(1, groups - 1)], q_recv)
    wait_bytes(kv_s.at[pl.ds(1, n - 1)], kv_recv)

    n_rows = n * rows_kv
    kv = kv_s[...].reshape(n_rows, LANES)
    if decoder:
        kvx_s[...] = kv
    else:
        bad = kv == jnp.inf
        kvx_s[:, :LANES] = jnp.where(bad, 0, kv).astype(jnp.bfloat16)
        kvx_s[:, LANES:] = jnp.where(bad & (lane_iota(kv.shape) == 0), NEG, 0.0).astype(jnp.bfloat16)

    per = bq // 16
    lane_sq = lane_iota((LANES, LANES))
    row_sq = lax.broadcasted_iota(jnp.int32, (LANES, LANES), 0)

    def send_o(k):
        to = lax.rem(me - 4 * k + n, n)
        pltpu.make_async_remote_copy(
            src_ref=o_s.at[k], dst_ref=om_ref.at[pair], send_sem=o_send, recv_sem=o_recv,
            device_id={'sp': to}, device_id_type=pl.DeviceIdType.MESH).start()

    def q_block(b, _):
        qp = q_s[pl.ds(b * per, per)].reshape(bq, LANES)
        if decoder:
            parts = []
            for half in range(2):
                for j in range(4):
                    pick = ((row_sq - 32 * j == lane_sq - 64 * half) & (lane_sq >= 64 * half) & (lane_sq < 64 * half + 32)).astype(jnp.bfloat16)
                    parts.append(jnp.dot(qp, pick, preferred_element_type=jnp.float32).astype(jnp.bfloat16))
            m, l, acc = flash(jnp.concatenate(parts, axis=0), kvx_s, n_rows, bk, scale)
            h = 4 * bq
            m_all = jnp.maximum(m[:h], m[h:])
            ea = jnp.exp2((m[:h] - m_all) * (scale * LOG2E))
            eb = jnp.exp2((m[h:] - m_all) * (scale * LOG2E))
            denom = l[:h] * ea + l[h:] * eb
            out = (acc[:h] * ea + pltpu.roll(acc[h:], 64, 1) * eb) / denom
            lane = lane_iota((bq, LANES))
            packed = jnp.zeros((bq, LANES), jnp.float32)
            for j in range(4):
                part = out[j * bq:(j + 1) * bq]
                moved = part if j == 1 else pltpu.roll(part, (32 * (j - 1)) % LANES, 1)
                packed = jnp.where((lane >= 32 * j) & (lane < 32 * j + 32), moved, packed)
        else:
            ones = (lane_iota((bq, LANES)) == 0).astype(jnp.bfloat16)
            m, l, acc = flash(jnp.concatenate([qp, ones], axis=1), kvx_s, n_rows, bk, scale)
            packed = acc / l
        o_s[pl.ds(b * per, per)] = packed.astype(jnp.bfloat16).reshape(per, 16, LANES)

        @pl.when(b > 0)
        def _():
            for r in range(per):
                k = (b - 1) * per + r

                @pl.when(k > 0)
                def _():
                    send_o(k)
        return 0

    n_blocks = groups // per
    lax.fori_loop(0, n_blocks, q_block, 0)
    om_ref[pair] = o_s[0]
    for r in range(per):
        send_o((n_blocks - 1) * per + r)

    rest = o_s.at[pl.ds(1, groups - 1)]
    wait_bytes(rest, o_recv)
    wait_bytes(rest, o_send)
    wait_bytes(q_s.at[pl.ds(1, groups - 1)], q_send)
    wait_bytes(kv_s.at[pl.ds(1, n - 1)], kv_send)


def exchange_attention(kvm, qm, n, decoder, scale, bq, bk):
    groups, rows_kv = kvm.shape[0], kvm.shape[1]
    n_keys = n * rows_kv
    width = LANES if decoder else 2 * LANES
    q_rows = groups * 16 * (8 if decoder else 1)
    vmem = pl.BlockSpec(memory_space=pltpu.VMEM)
    return pl.pallas_call(
        functools.partial(attention_kernel, n, rows_kv, decoder, scale, bq, bk),
        out_shape=jax.ShapeDtypeStruct((groups, 16, LANES), jnp.bfloat16),
        in_specs=[vmem, vmem],
        out_specs=vmem,
        scratch_shapes=[
            pltpu.VMEM((n, rows_kv, LANES), jnp.bfloat16),
            pltpu.VMEM((groups, 16, LANES), jnp.bfloat16),
            pltpu.VMEM((groups, 16, LANES), jnp.bfloat16),
            pltpu.VMEM((n_keys, width), jnp.bfloat16),
        ] + [pltpu.SemaphoreType.DMA] * 6,
        compiler_params=pltpu.CompilerParams(
            collective_id=0 if decoder else 1, has_side_effects=True, vmem_limit_bytes=48 * 1024 * 1024),
        cost_estimate=pl.CostEstimate(flops=4 * q_rows * n_keys * LANES, bytes_accessed=2 * n_keys * LANES * 2, transcendentals=q_rows * n_keys),
        name='dec_attention' if decoder else 'enc_attention',
    )(kvm, qm)


def mlp(mid_state, w_up, w_down):
    up_act = jax.nn.gelu(jnp.dot(layer_norm(mid_state), w_up, preferred_element_type=jnp.float32), approximate=False).astype(jnp.bfloat16)
    return (mid_state + jnp.dot(up_act, w_down, preferred_element_type=jnp.float32)).astype(jnp.bfloat16)


def enc_block(hidden, valid, w_qkv, w_proj, w_up, w_down, n):
    clips, slots = valid.shape
    heads, hd = w_qkv.shape[2], w_qkv.shape[3]
    d = heads * hd
    qkv = jnp.dot(layer_norm(hidden), w_qkv.reshape(d, 3 * d), preferred_element_type=jnp.float32).astype(jnp.bfloat16)
    qkv = qkv.reshape(clips, slots, 3, heads, hd)
    kv = jnp.concatenate([qkv[:, :, 1], qkv[:, :, 2]], axis=-1)
    kv = jnp.where(valid[:, :, None, None], kv, jnp.inf).transpose(0, 2, 1, 3).reshape(clips * heads, slots, LANES)
    q = jnp.pad(qkv[:, :, 0], ((0, 0), (0, 0), (0, 0), (0, LANES - hd))).transpose(0, 2, 1, 3).reshape(clips * heads, slots, LANES)
    om = exchange_attention(kv, q, n, False, hd ** -0.5, 256, 1024)
    att = om.reshape(clips, heads, slots, LANES)[:, :, :, hd:].transpose(0, 2, 1, 3).reshape(clips * slots, d)
    mid = (hidden + jnp.dot(att, w_proj.reshape(d, d), preferred_element_type=jnp.float32)).astype(jnp.bfloat16)
    return mlp(mid, w_up, w_down)


def dec_block(hidden, clips, w_qkv, w_proj, w_up, w_down, n):
    rows = hidden.shape[0] // clips
    heads, hd = w_qkv.shape[2], w_qkv.shape[3]
    d = heads * hd
    qkv = jnp.dot(layer_norm(hidden), w_qkv.reshape(d, 3 * d), preferred_element_type=jnp.float32).astype(jnp.bfloat16)
    qkv = qkv.reshape(clips, rows, 3, heads, hd)
    kv = jnp.concatenate([qkv[:, :, 1], qkv[:, :, 2]], axis=-1)
    kv = kv.reshape(clips, 2, rows // 2, heads, 2 * hd).transpose(0, 3, 2, 1, 4).reshape(clips * heads, rows // 2, LANES)
    q = qkv[:, :, 0].reshape(clips, 4, rows // 4, heads, hd).transpose(0, 3, 2, 1, 4).reshape(clips * heads, rows // 4, LANES)
    om = exchange_attention(kv, q, n, True, hd ** -0.5, 64, 1024)
    att = om.reshape(clips, heads, rows // 4, 4, hd).transpose(0, 3, 2, 1, 4).reshape(clips * rows, d)
    mid = (hidden + jnp.dot(att, w_proj.reshape(d, d), preferred_element_type=jnp.float32)).astype(jnp.bfloat16)
    return mlp(mid, w_up, w_down)


def solution(mesh):
    n = mesh.shape['sp']

    def local_program(patches, vis_mask, enc_pos, dec_pos, w_pe, b_pe, enc_qkv, enc_proj, enc_up, enc_down, w_ed, mask_token, dec_qkv, dec_proj, dec_up, dec_down, w_out):
        clips, tokens = vis_mask.shape
        slots = 2 * (tokens // KEEP_DIV)
        upto = (jnp.arange(tokens)[:, None] < jnp.arange(tokens)[None, :]).astype(jnp.float32)
        local_rank = jnp.dot(vis_mask.astype(jnp.float32), upto).astype(jnp.int32)
        count = jnp.sum(vis_mask, axis=1)
        valid = jnp.arange(slots)[None, :] < count[:, None]
        select = ((local_rank[:, None, :] == jnp.arange(slots)[None, :, None]) & (vis_mask[:, None, :] == 1)).astype(jnp.bfloat16)
        moved_x = jnp.einsum('cqi,cip->cqp', select, patches, preferred_element_type=jnp.float32).astype(jnp.bfloat16)
        moved_pos = jnp.einsum('cqi,id->cqd', select, enc_pos, preferred_element_type=jnp.float32)
        hidden = (jnp.einsum('cqp,pd->cqd', moved_x, w_pe, preferred_element_type=jnp.float32)
                  + b_pe.astype(jnp.float32) + moved_pos).astype(jnp.bfloat16).reshape(clips * slots, -1)
        for layer in range(enc_qkv.shape[0]):
            hidden = enc_block(hidden, valid, enc_qkv[layer], enc_proj[layer], enc_up[layer], enc_down[layer], n)
        z = jnp.dot(layer_norm(hidden), w_ed, preferred_element_type=jnp.float32).astype(jnp.bfloat16)
        placed = jnp.einsum('cqi,cqe->cie', select, z.reshape(clips, slots, -1), preferred_element_type=jnp.float32)
        masked_part = (1 - vis_mask).astype(jnp.float32)[:, :, None] * mask_token.astype(jnp.float32)
        hidden = (placed + masked_part + dec_pos.astype(jnp.float32)).astype(jnp.bfloat16).reshape(clips * tokens, -1)
        for layer in range(dec_qkv.shape[0]):
            hidden = dec_block(hidden, clips, dec_qkv[layer], dec_proj[layer], dec_up[layer], dec_down[layer], n)
        return jnp.dot(layer_norm(hidden), w_out, preferred_element_type=jnp.float32).reshape(clips, tokens, -1)

    row_spec = P('dp', 'sp', None)
    pos_spec = P(('dp', 'sp'), None)
    arg_specs = (row_spec, P('dp', 'sp'), pos_spec, pos_spec) + (P(),) * 13
    return jax.shard_map(local_program, mesh=mesh, in_specs=arg_specs, out_specs=row_spec, check_vma=False)
```

```python
import functools

import jax
import jax.numpy as jnp
from jax import lax
from jax.experimental import pallas as pl
from jax.experimental.pallas import tpu as pltpu
from jax.sharding import PartitionSpec as P

KEEP_DIV = 8
LANES = 128
QUARTERS = 4
MSG = 16
LOG2E = 1.4426950408889634
NEG = -3e38
BF16 = jnp.bfloat16
F32 = jnp.float32


def layer_norm(hidden):
    hid_f32 = hidden.astype(F32)
    centred = hid_f32 - jnp.mean(hid_f32, axis=-1, keepdims=True)
    row_var = jnp.mean(centred * centred, axis=-1, keepdims=True)
    return (centred * lax.rsqrt(row_var + 1e-6)).astype(BF16)


def gelu(x):
    return 0.5 * x * (1.0 + lax.erf(x * (0.5 ** 0.5)))


def dot(a, b):
    return jnp.dot(a, b, preferred_element_type=F32)


def dot_t(a, b):
    return lax.dot_general(a, b, (((1,), (1,)), ((), ())), preferred_element_type=F32)


def lane_of(shape):
    return lax.broadcasted_iota(jnp.int32, shape, len(shape) - 1)


def roll(x, shift):
    shift = shift % LANES
    return x if shift == 0 else pltpu.roll(x, shift, 1)


def wait_bytes(ref, sem):
    pltpu.make_async_copy(ref, ref, sem).wait()


def model_kernel(n, enc_heads, dec_heads, patches, mask, enc_pos, dec_pos, b_pe, mask_token,
                 w_pe, e_qkv, e_proj, e_up, e_down, w_ed, d_qkv, d_proj, d_up, d_down, w_out, out,
                 w_pe_s, e_qkv_s, e_proj_s, e_up_s, e_down_s, w_ed_s, d_qkv_s, d_proj_s, d_up_s, d_down_s, w_out_s,
                 ekvm, dkvm, qm, o_s, ekv, dkv, q_in, o_in, ekvx, kvt, qq, s_buf, p_buf, hid_e, qkv_e, att_e, hid_d, qkv_d, att_d, pick_s,
                 wsem, kv_send, kv_recv, q_send, q_recv, o_send, o_recv):
    me = lax.axis_index('sp')
    groups = n // QUARTERS
    pair = me // QUARTERS
    clips, tokens, _ = patches.shape
    slots = 2 * (tokens // KEEP_DIV)
    layers = e_qkv.shape[0]
    d_enc = enc_pos.shape[1]
    d_dec = dec_pos.shape[1]
    mesh_id = pl.DeviceIdType.MESH

    def load(src, dst, i):
        return pltpu.make_async_copy(src, dst, wsem.at[i])

    load_pe = load(w_pe, w_pe_s, 0)
    load_ed = load(w_ed, w_ed_s, 5)
    load_out = load(w_out, w_out_s, 10)
    enc_loads = [(e_qkv, e_qkv_s, 1), (e_proj, e_proj_s, 2), (e_up, e_up_s, 3), (e_down, e_down_s, 4)]
    dec_loads = [load(d_qkv, d_qkv_s, 6), load(d_proj, d_proj_s, 7), load(d_up, d_up_s, 8), load(d_down, d_down_s, 9)]

    def enc_load(which, layer):
        src, dst, i = enc_loads[which]
        return load(src.at[layer], dst, i)

    load_pe.start()
    enc_load(0, 0).start()

    barrier = pltpu.get_barrier_semaphore()

    def greet(i, _):
        pl.semaphore_signal(barrier, inc=1, device_id={'sp': lax.rem(me + i, n)}, device_id_type=mesh_id)
        return 0

    lax.fori_loop(1, n, greet, 0)

    mask_f = mask[...].astype(F32)
    before = lax.broadcasted_iota(jnp.int32, (tokens, tokens), 0) < lax.broadcasted_iota(jnp.int32, (tokens, tokens), 1)
    rank = dot(mask_f.astype(BF16), before.astype(BF16))
    slot_id = lax.broadcasted_iota(jnp.int32, (slots, tokens), 0).astype(F32)
    selects, moved_x, moved_pos, occupied = [], [], [], []
    for c in range(clips):
        select = jnp.where((rank[c:c + 1] == slot_id) & (mask_f[c:c + 1] > 0), 1.0, 0.0)
        selects.append(select)
        moved_x.append(dot(select.astype(BF16), patches[c]).astype(BF16))
        moved_pos.append(dot(select.astype(BF16), enc_pos[...]))
        occupied.append(jnp.sum(select, axis=1, keepdims=True))
    load_pe.wait()
    embedded = dot(jnp.concatenate(moved_x, axis=0), w_pe_s[...]) + b_pe[...].astype(F32) + jnp.concatenate(moved_pos, axis=0)
    hid_e[...] = embedded.astype(BF16)
    for which in range(1, 4):
        enc_load(which, 0).start()
    pl.semaphore_wait(barrier, n - 1)

    def exchange(phase, kvm, kv):
        def send_kv(i, _):
            to = lax.rem(me + i, n)
            pltpu.make_async_remote_copy(
                src_ref=kvm.at[to // QUARTERS], dst_ref=kv.at[i], send_sem=kv_send.at[phase], recv_sem=kv_recv.at[phase],
                device_id={'sp': to}, device_id_type=mesh_id).start()
            return 0

        def send_q(k, _):
            to = lax.rem(me + QUARTERS * k, n)
            pltpu.make_async_remote_copy(
                src_ref=qm.at[to // QUARTERS], dst_ref=q_in.at[phase, k], send_sem=q_send.at[phase], recv_sem=q_recv.at[phase],
                device_id={'sp': to}, device_id_type=mesh_id).start()
            return 0

        lax.fori_loop(1, groups, send_q, 0)
        lax.fori_loop(1, n, send_kv, 0)
        q_in[phase, 0] = qm[pair]
        kv[0] = kvm[pair]

    def arrived(phase, kv):
        wait_bytes(q_in.at[phase, pl.ds(1, groups - 1)], q_recv.at[phase])
        wait_bytes(kv.at[pl.ds(1, n - 1)], kv_recv.at[phase])

    def send_home(phase, k):
        to = lax.rem(me - QUARTERS * k + n, n)
        pltpu.make_async_remote_copy(
            src_ref=o_s.at[k], dst_ref=o_in.at[phase, pair], send_sem=o_send.at[phase], recv_sem=o_recv.at[phase],
            device_id={'sp': to}, device_id_type=mesh_id).start()

    def finish(phase, kv):
        rest = pl.ds(1, groups - 1)
        wait_bytes(o_in.at[phase, rest], o_recv.at[phase])
        wait_bytes(o_s.at[rest], o_send.at[phase])
        wait_bytes(qm.at[rest], q_send.at[phase])
        wait_bytes(kv.at[pl.ds(1, n - 1)], kv_send.at[phase])

    hd_e = d_enc // enc_heads
    lane_e = lane_of((slots, LANES))
    c_e = hd_e ** -0.5 * LOG2E
    n_e = n * slots
    m_e = groups * slots
    bk = 256

    def enc_layer(layer, _):
        normed = layer_norm(hid_e[...])
        enc_load(0, layer).wait()
        for t in range(0, 3 * d_enc, 1024):
            qkv_e[:, t:t + 1024] = dot_t(normed, e_qkv_s[t:t + 1024])

        @pl.when(layer + 1 < layers)
        def _():
            enc_load(0, layer + 1).start()

        for c in range(clips):
            rows = slice(c * slots, (c + 1) * slots)
            for h in range(enc_heads):
                tile = (h * hd_e) // LANES * LANES
                off = h * hd_e - tile
                q_t = roll(qkv_e[rows, tile:tile + LANES], -off)
                k_t = roll(qkv_e[rows, d_enc + tile:d_enc + tile + LANES], -off)
                v_t = roll(qkv_e[rows, 2 * d_enc + tile:2 * d_enc + tile + LANES], hd_e - off)
                qm[c * enc_heads + h] = jnp.where(lane_e < hd_e, q_t, 0.0).astype(BF16)
                kv_t = jnp.where(lane_e < hd_e, k_t, v_t)
                ekvm[c * enc_heads + h] = jnp.where(occupied[c] > 0, kv_t, jnp.inf).astype(BF16)

        kv = ekv.at[layer]
        exchange(layer, ekvm, kv)

        @pl.when(layer == 0)
        def _():
            load_ed.start()
            for copy in dec_loads:
                copy.start()
            load_out.start()

        arrived(layer, kv)
        for t in range(0, n, 32):
            block = kv[t:t + 32].reshape(32 * slots, LANES)
            bad = block == jnp.inf
            r = slice(t * slots, (t + 32) * slots)
            clean = jnp.where(bad, jnp.zeros_like(block), block)
            ekvx[r, :LANES] = clean
            ekvx[r, LANES:] = jnp.where(bad & (lane_of(block.shape) == 0), jnp.full_like(block, NEG), jnp.zeros_like(block))
            kvt[:, r] = clean.T
        q = q_in[layer].reshape(m_e, LANES)
        q = jnp.concatenate([q, (lane_of(q.shape) == 0).astype(BF16)], axis=1)
        steps = n_e // bk
        m = jnp.full((1, m_e), NEG, F32)
        l = jnp.zeros((1, m_e), F32)
        acc = jnp.zeros((hd_e, m_e), F32)
        s_buf[0, :, :m_e] = dot_t(ekvx[:bk], q)
        prev = None
        for i in range(steps):
            if i + 1 < steps:
                s_buf[(i + 1) % 2, :, :m_e] = dot_t(ekvx[(i + 1) * bk:(i + 2) * bk], q)
            s = s_buf[i % 2, :, :m_e]
            m_new = jnp.maximum(m, jnp.max(s, axis=0, keepdims=True))
            p = jnp.exp2(s * c_e - m_new * c_e)
            alpha = jnp.exp2((m - m_new) * c_e)
            l = l * alpha + jnp.sum(p, axis=0, keepdims=True)
            p_buf[i % 2, :, :m_e] = p.astype(BF16)
            m = m_new
            if prev is not None:
                j, a = prev
                acc = acc * a + dot(kvt[hd_e:2 * hd_e, j * bk:(j + 1) * bk], p_buf[j % 2, :, :m_e])
            prev = (i, alpha)
        j, a = prev
        acc = acc * a + dot(kvt[hd_e:2 * hd_e, j * bk:(j + 1) * bk], p_buf[j % 2, :, :m_e])
        res = acc / l
        odd = lax.rem(pair, 2) == 1
        zero = jnp.zeros_like(res)
        both = jnp.concatenate([jnp.where(odd, zero, res), jnp.where(odd, res, zero)], axis=0)
        o_s[...] = both.T.astype(BF16).reshape(groups, slots, LANES)

        def home(k, _):
            send_home(layer, k)
            return 0

        o_in[layer, pair] = o_s[0]
        lax.fori_loop(1, groups, home, 0)
        finish(layer, kv)

        for c in range(clips):
            for g in range(enc_heads // 2):
                first = c * enc_heads + 2 * g
                att_e[c * slots:(c + 1) * slots, g * LANES:(g + 1) * LANES] = (
                    o_in[layer, first].astype(F32) + o_in[layer, first + 1].astype(F32)).astype(BF16)
        enc_load(1, layer).wait()
        mid = (hid_e[...].astype(F32) + dot(att_e[...], e_proj_s[...])).astype(BF16)

        @pl.when(layer + 1 < layers)
        def _():
            enc_load(1, layer + 1).start()

        normed = layer_norm(mid)
        enc_load(2, layer).wait()
        enc_load(3, layer).wait()
        total = mid.astype(F32)
        for t in range(0, e_up_s.shape[1], 1024):
            up = gelu(dot(normed, e_up_s[:, t:t + 1024])).astype(BF16)
            total = total + dot(up, e_down_s[t:t + 1024])

        @pl.when(layer + 1 < layers)
        def _():
            enc_load(2, layer + 1).start()
            enc_load(3, layer + 1).start()

        hid_e[...] = total.astype(BF16)
        return 0

    lax.fori_loop(0, layers, enc_layer, 0)

    load_ed.wait()
    z = dot(layer_norm(hid_e[...]), w_ed_s[...]).astype(BF16)
    for c in range(clips):
        placed = lax.dot_general(selects[c].astype(BF16), z[c * slots:(c + 1) * slots], (((0,), (0,)), ((), ())), preferred_element_type=F32)
        seen = jnp.max(selects[c].T, axis=1, keepdims=True)
        token = jnp.where(seen > 0, placed, mask_token[...].astype(F32))
        hid_d[c * tokens:(c + 1) * tokens] = (token + dec_pos[...].astype(F32)).astype(BF16)

    hd_d = d_dec // dec_heads
    c_d = hd_d ** -0.5 * LOG2E
    half = tokens // 2
    parts = LANES // hd_d
    rows_q = tokens // parts
    n_d = n * half
    q_rows = groups * rows_q
    blk = 128
    m_d = 2 * parts * blk
    h_d = m_d // 2
    per = blk // rows_q
    lane_q = lane_of((rows_q, LANES))
    lane_k = lane_of((half, LANES))
    col = lane_of((LANES, 2 * parts * LANES))
    row = lax.broadcasted_iota(jnp.int32, col.shape, 0)
    part = col // LANES
    inside = lax.rem(col, LANES) - jnp.where(part >= parts, 2 * hd_d, 0)
    pick_s[...] = jnp.where((inside >= 0) & (inside < hd_d) & (row == inside + hd_d * lax.rem(part, parts)), 1.0, 0.0).astype(BF16)
    for copy in dec_loads:
        copy.wait()

    def dec_layer(layer, _):
        phase = layers + layer
        normed = layer_norm(hid_d[...])
        qkv_d[...] = dot_t(normed, d_qkv_s[layer])
        for c in range(clips):
            base = c * tokens
            for h in range(dec_heads):
                tile = (h * hd_d) // LANES * LANES
                off = h * hd_d - tile
                lo = slice(base, base + half)
                hi = slice(base + half, base + tokens)
                kc = slice(d_dec + tile, d_dec + tile + LANES)
                vc = slice(2 * d_dec + tile, 2 * d_dec + tile + LANES)
                k_lo, v_lo = roll(qkv_d[lo, kc], -off), roll(qkv_d[lo, vc], hd_d - off)
                k_hi, v_hi = roll(qkv_d[hi, kc], 2 * hd_d - off), roll(qkv_d[hi, vc], 3 * hd_d - off)
                dkvm[c * dec_heads + h] = jnp.where(
                    lane_k < 2 * hd_d, jnp.where(lane_k < hd_d, k_lo, v_lo), jnp.where(lane_k < 3 * hd_d, k_hi, v_hi)).astype(BF16)
                packed = None
                for j in range(parts):
                    moved = roll(qkv_d[base + j * rows_q:base + (j + 1) * rows_q, tile:tile + LANES], hd_d * j - off)
                    packed = moved if packed is None else jnp.where(lane_q >= hd_d * j, moved, packed)
                qm[c * dec_heads + h] = packed.astype(BF16)
        kv = dkv.at[layer]
        exchange(phase, dkvm, kv)
        arrived(phase, kv)

        spread = dot(q_in[phase].reshape(q_rows, LANES), pick_s[...])
        for b in range(q_rows // blk):
            for t in range(2 * parts):
                qq[b * m_d + t * blk:b * m_d + (t + 1) * blk] = spread[b * blk:(b + 1) * blk, t * LANES:(t + 1) * LANES].astype(BF16)
        for t in range(0, n, 16):
            kvt[:, t * half:(t + 16) * half] = kv[t:t + 16].reshape(16 * half, LANES).T

        steps = n_d // bk
        msgs = bk // half
        blocks = q_rows // blk

        def scores(b, i, slot):
            q = qq[pl.ds(pl.multiple_of(b * m_d, m_d), m_d)]
            s_buf[slot] = dot_t(kv[i * msgs:(i + 1) * msgs].reshape(bk, LANES), q)

        scores(0, 0, 0)

        def q_block(b, _):
            m = jnp.full((1, m_d), NEG, F32)
            l = jnp.zeros((1, m_d), F32)
            acc_a = jnp.zeros((hd_d, h_d), F32)
            acc_b = jnp.zeros((hd_d, h_d), F32)
            alphas = []

            def add(i, acc_a, acc_b):
                keys = slice(i * bk, (i + 1) * bk)
                acc_a = acc_a * alphas[i][:, :h_d] + dot(kvt[hd_d:2 * hd_d, keys], p_buf[i % 2, :, :h_d])
                acc_b = acc_b * alphas[i][:, h_d:] + dot(kvt[3 * hd_d:4 * hd_d, keys], p_buf[i % 2, :, h_d:])
                return acc_a, acc_b

            for i in range(steps):
                if i + 1 < steps:
                    scores(b, i + 1, (i + 1) % 2)
                else:
                    scores(jnp.minimum(b + 1, blocks - 1), 0, 0)
                s = s_buf[i % 2]
                m_new = jnp.maximum(m, jnp.max(s, axis=0, keepdims=True))
                p = jnp.exp2(s * c_d - m_new * c_d)
                alphas.append(jnp.exp2((m - m_new) * c_d))
                l = l * alphas[i] + jnp.sum(p, axis=0, keepdims=True)
                p_buf[i % 2] = p.astype(BF16)
                m = m_new
                if i > 0:
                    acc_a, acc_b = add(i - 1, acc_a, acc_b)
            acc_a, acc_b = add(steps - 1, acc_a, acc_b)
            m_all = jnp.maximum(m[:, :h_d], m[:, h_d:])
            e_a = jnp.exp2((m[:, :h_d] - m_all) * c_d)
            e_b = jnp.exp2((m[:, h_d:] - m_all) * c_d)
            res = (acc_a * e_a + acc_b * e_b) / (l[:, :h_d] * e_a + l[:, h_d:] * e_b)
            stacked = jnp.concatenate([res[:, j * blk:(j + 1) * blk] for j in range(parts)], axis=0)
            o_s[pl.ds(b * per, per)] = stacked.T.astype(BF16).reshape(per, rows_q, LANES)

            def home(k, _):
                send_home(phase, k)
                return 0

            lax.fori_loop(jnp.maximum(b * per, 1), (b + 1) * per, home, 0)
            return 0

        lax.fori_loop(0, blocks, q_block, 0)
        o_in[phase, pair] = o_s[0]
        finish(phase, kv)

        for c in range(clips):
            for g in range(dec_heads // parts):
                got = [o_in[phase, c * dec_heads + parts * g + h].astype(F32) for h in range(parts)]
                for j in range(parts):
                    tile = None
                    for h in range(parts):
                        moved = roll(got[h], hd_d * (h - j))
                        tile = moved if tile is None else jnp.where(lane_q >= hd_d * h, moved, tile)
                    att_d[c * tokens + j * rows_q:c * tokens + (j + 1) * rows_q, g * LANES:(g + 1) * LANES] = tile.astype(BF16)
        mid = (hid_d[...].astype(F32) + dot(att_d[...], d_proj_s[layer])).astype(BF16)
        up = gelu(dot(layer_norm(mid), d_up_s[layer])).astype(BF16)
        hid_d[...] = (mid.astype(F32) + dot(up, d_down_s[layer])).astype(BF16)
        return 0

    lax.fori_loop(0, layers, dec_layer, 0)
    load_out.wait()
    result = dot(layer_norm(hid_d[...]), w_out_s[...])
    for c in range(clips):
        out[c] = result[c * tokens:(c + 1) * tokens]


def solution(mesh):
    n = mesh.shape['sp']

    def local_program(patches, vis_mask, enc_pos, dec_pos, w_pe, b_pe, enc_qkv, enc_proj, enc_up, enc_down, w_ed, mask_token, dec_qkv, dec_proj, dec_up, dec_down, w_out):
        clips, tokens, width = patches.shape
        layers, d_enc, _, enc_heads, _ = enc_qkv.shape
        _, d_dec, _, dec_heads, _ = dec_qkv.shape
        slots = 2 * (tokens // KEEP_DIV)
        half = tokens // 2
        groups = n // QUARTERS
        f_enc, f_dec = enc_up.shape[2], dec_up.shape[2]
        e_rows, d_rows = clips * slots, clips * tokens
        phases = 2 * layers
        bk, m_d = 256, 1024
        vmem = pl.BlockSpec(memory_space=pltpu.VMEM)
        hbm = pl.BlockSpec(memory_space=pl.ANY)

        def buf(*shape, dtype=BF16):
            return pltpu.VMEM(shape, dtype)

        return pl.pallas_call(
            functools.partial(model_kernel, n, enc_heads, dec_heads),
            out_shape=jax.ShapeDtypeStruct((clips, tokens, w_out.shape[1]), F32),
            in_specs=[vmem] * 6 + [hbm] * 11,
            out_specs=vmem,
            scratch_shapes=[
                buf(width, d_enc), buf(3 * d_enc, d_enc), buf(d_enc, d_enc), buf(d_enc, f_enc), buf(f_enc, d_enc), buf(d_enc, d_dec),
                buf(layers, 3 * d_dec, d_dec), buf(layers, d_dec, d_dec), buf(layers, d_dec, f_dec), buf(layers, f_dec, d_dec), buf(d_dec, w_out.shape[1]),
                buf(groups, slots, LANES), buf(groups, half, LANES), buf(groups, MSG, LANES), buf(groups, MSG, LANES),
                buf(layers, n, slots, LANES), buf(layers, n, half, LANES), buf(phases, groups, MSG, LANES), buf(phases, groups, MSG, LANES),
                buf(n * slots, 2 * LANES), buf(LANES, n * half), buf(groups * MSG * 8, LANES),
                buf(2, bk, m_d, dtype=F32), buf(2, bk, m_d),
                buf(e_rows, d_enc), buf(e_rows, 3 * d_enc, dtype=F32), buf(e_rows, d_enc),
                buf(d_rows, d_dec), buf(d_rows, 3 * d_dec, dtype=F32), buf(d_rows, d_dec),
                buf(LANES, 8 * LANES),
                pltpu.SemaphoreType.DMA((11,)),
            ] + [pltpu.SemaphoreType.DMA((phases,))] * 6,
            compiler_params=pltpu.CompilerParams(collective_id=0, has_side_effects=True, vmem_limit_bytes=67043328),
            name='model',
        )(patches, vis_mask, enc_pos, dec_pos, b_pe.reshape(1, -1), mask_token.reshape(1, -1), w_pe,
          enc_qkv.transpose(0, 2, 3, 4, 1).reshape(layers, 3 * d_enc, d_enc), enc_proj.reshape(layers, d_enc, d_enc), enc_up, enc_down, w_ed,
          dec_qkv.transpose(0, 2, 3, 4, 1).reshape(layers, 3 * d_dec, d_dec), dec_proj.reshape(layers, d_dec, d_dec), dec_up, dec_down, w_out)

    row_spec = P('dp', 'sp', None)
    pos_spec = P(('dp', 'sp'), None)
    arg_specs = (row_spec, P('dp', 'sp'), pos_spec, pos_spec) + (P(),) * 13
    return jax.shard_map(local_program, mesh=mesh, in_specs=arg_specs, out_specs=row_spec, check_vma=False)
```

```python
import functools

import jax
import jax.numpy as jnp
from jax import lax
from jax.experimental import pallas as pl
from jax.experimental.pallas import tpu as pltpu
from jax.sharding import PartitionSpec as P

KEEP_DIV = 8
LANES = 128
QUARTERS = 4
MSG = 16
LOG2E = 1.4426950408889634
NEG = -3e38
SIDE = 4
CHUNKS = 4
BF16 = jnp.bfloat16
F32 = jnp.float32


def layer_norm(hidden):
    hid_f32 = hidden.astype(F32)
    centred = hid_f32 - jnp.mean(hid_f32, axis=-1, keepdims=True)
    row_var = jnp.mean(centred * centred, axis=-1, keepdims=True)
    return (centred * lax.rsqrt(row_var + 1e-6)).astype(BF16)


def gelu(x):
    return 0.5 * x * (1.0 + lax.erf(x * (0.5 ** 0.5)))


def dot(a, b):
    return jnp.dot(a, b, preferred_element_type=F32)


def dot_t(a, b):
    return lax.dot_general(a, b, (((1,), (1,)), ((), ())), preferred_element_type=F32)


def lane_of(shape):
    return lax.broadcasted_iota(jnp.int32, shape, len(shape) - 1)


def roll(x, shift):
    shift = shift % LANES
    return x if shift == 0 else pltpu.roll(x, shift, 1)


def wait_bytes(ref, sem):
    pltpu.make_async_copy(ref, ref, sem).wait()


def model_kernel(n, enc_heads, dec_heads, patches, mask, enc_pos, dec_pos, b_pe, mask_token,
                 w_pe, e_qkv, e_proj, e_up, e_down, w_ed, d_qkv, d_proj, d_up, d_down, w_out, out,
                 w_pe_s, e_qkv_s, e_proj_s, e_up_s, e_down_s, w_ed_s, d_qkv_s, d_proj_s, d_up_s, d_down_s, w_out_s,
                 ekvm, dkvm, qm, o_s, ekv, dkv, q_in, o_in, ekvx, kvt, qq, s_buf, p_buf, hid_e, qkv_e, att_e, hid_d, qkv_d, att_d, pick_s,
                 m_st, l_st, acc_st, wsem, kv_send, kv_recv, f_send, f_recv, q_send, q_recv, o_send, o_recv):
    me = lax.axis_index('sp')
    groups = n // QUARTERS
    pair = me // QUARTERS
    chips = n // 2
    per_chunk = chips // CHUNKS
    core = lax.rem(me, 2)
    partner = me + 1 - 2 * core
    at_z, at_y, at_x = me // 32, lax.rem(me // 8, SIDE), lax.rem(me // 2, SIDE)

    def device_at(dz, dy, dx):
        return (lax.rem(at_z + dz, SIDE) * SIDE + lax.rem(at_y + dy, SIDE)) * 8 + lax.rem(at_x + dx, SIDE) * 2 + core

    far = {0: 0, 1: 1, 2: 2, 3: 1}
    offsets = sorted(((dz, dy, dx) for dz in range(SIDE) for dy in range(SIDE) for dx in range(SIDE)), key=lambda o: far[o[0]] + far[o[1]] + far[o[2]])

    def query_offset(block, j):
        return 2 * lax.rem(block, 2) + j // 4, j % 4, 2 * (block // 2)

    def back(d):
        return SIDE - d
    clips, tokens, _ = patches.shape
    slots = 2 * (tokens // KEEP_DIV)
    layers = e_qkv.shape[0]
    d_enc = enc_pos.shape[1]
    d_dec = dec_pos.shape[1]
    mesh_id = pl.DeviceIdType.MESH

    def load(src, dst, i):
        return pltpu.make_async_copy(src, dst, wsem.at[i])

    load_pe = load(w_pe, w_pe_s, 0)
    load_ed = load(w_ed, w_ed_s, 5)
    load_out = load(w_out, w_out_s, 10)
    enc_loads = [(e_qkv, e_qkv_s, 1), (e_proj, e_proj_s, 2), (e_up, e_up_s, 3), (e_down, e_down_s, 4)]
    dec_loads = [load(d_qkv, d_qkv_s, 6), load(d_proj, d_proj_s, 7), load(d_up, d_up_s, 8), load(d_down, d_down_s, 9)]

    def enc_load(which, layer):
        src, dst, i = enc_loads[which]
        return load(src.at[layer], dst, i)

    load_pe.start()
    enc_load(0, 0).start()

    barrier = pltpu.get_barrier_semaphore()

    def greet(i, _):
        pl.semaphore_signal(barrier, inc=1, device_id={'sp': lax.rem(me + 2 * i, n)}, device_id_type=mesh_id)
        return 0

    lax.fori_loop(1, chips, greet, 0)
    pl.semaphore_signal(barrier, inc=1, device_id={'sp': partner}, device_id_type=mesh_id)

    mask_f = mask[...].astype(F32)
    before = lax.broadcasted_iota(jnp.int32, (tokens, tokens), 0) < lax.broadcasted_iota(jnp.int32, (tokens, tokens), 1)
    rank = dot(mask_f.astype(BF16), before.astype(BF16))
    slot_id = lax.broadcasted_iota(jnp.int32, (slots, tokens), 0).astype(F32)
    selects, moved_x, moved_pos, occupied = [], [], [], []
    for c in range(clips):
        select = jnp.where((rank[c:c + 1] == slot_id) & (mask_f[c:c + 1] > 0), 1.0, 0.0)
        selects.append(select)
        moved_x.append(dot(select.astype(BF16), patches[c]).astype(BF16))
        moved_pos.append(dot(select.astype(BF16), enc_pos[...]))
        occupied.append(jnp.sum(select, axis=1, keepdims=True))
    load_pe.wait()
    embedded = dot(jnp.concatenate(moved_x, axis=0), w_pe_s[...]) + b_pe[...].astype(F32) + jnp.concatenate(moved_pos, axis=0)
    hid_e[...] = embedded.astype(BF16)
    for which in range(1, 4):
        enc_load(which, 0).start()

    def exchange(phase, kvm, kv):
        for k in range(1, groups):
            to = device_at(*query_offset(k // 8, k % 8))
            pltpu.make_async_remote_copy(
                src_ref=qm.at[to // QUARTERS], dst_ref=q_in.at[phase, k], send_sem=q_send.at[phase], recv_sem=q_recv.at[phase],
                device_id={'sp': to}, device_id_type=mesh_id).start()
        for i in range(1, chips):
            to = device_at(*offsets[i])
            pltpu.make_async_remote_copy(
                src_ref=kvm.at[to // QUARTERS], dst_ref=kv.at[i], send_sem=kv_send.at[phase], recv_sem=kv_recv.at[phase, i // per_chunk],
                device_id={'sp': to}, device_id_type=mesh_id).start()
        q_in[phase, 0] = qm[pair]
        kv[0] = kvm[pair]

    def relay(phase, kv, c):
        first = 1 if c == 0 else 0
        wait_bytes(kv.at[pl.ds(c * per_chunk + first, per_chunk - first)], kv_recv.at[phase, c])
        pltpu.make_async_remote_copy(
            src_ref=kv.at[pl.ds(c * per_chunk, per_chunk)], dst_ref=kv.at[pl.ds(chips + c * per_chunk, per_chunk)],
            send_sem=f_send.at[phase], recv_sem=f_recv.at[phase, c], device_id={'sp': partner}, device_id_type=mesh_id).start()

    def relayed(phase, kv, c):
        wait_bytes(kv.at[pl.ds(chips + c * per_chunk, per_chunk)], f_recv.at[phase, c])

    def queries_in(phase):
        wait_bytes(q_in.at[phase, pl.ds(1, groups - 1)], q_recv.at[phase])

    def send_home(phase, block, j):
        dz, dy, dx = query_offset(block, j)
        to = device_at(back(dz), back(dy), back(dx))
        pltpu.make_async_remote_copy(
            src_ref=o_s.at[8 * block + j], dst_ref=o_in.at[phase, pair], send_sem=o_send.at[phase], recv_sem=o_recv.at[phase],
            device_id={'sp': to}, device_id_type=mesh_id).start()

    def finish(phase, kv):
        rest = pl.ds(1, groups - 1)
        wait_bytes(o_in.at[phase, rest], o_recv.at[phase])
        wait_bytes(o_s.at[rest], o_send.at[phase])
        wait_bytes(qm.at[rest], q_send.at[phase])
        wait_bytes(kv.at[pl.ds(1, chips - 1)], kv_send.at[phase])
        wait_bytes(kv.at[pl.ds(0, chips)], f_send.at[phase])

    hd_e = d_enc // enc_heads
    lane_e = lane_of((slots, LANES))
    c_e = hd_e ** -0.5 * LOG2E
    n_e = n * slots
    m_e = groups * slots
    bk = 256

    def enc_layer(layer, _):
        normed = layer_norm(hid_e[...])
        enc_load(0, layer).wait()
        for t in range(0, 3 * d_enc, 1024):
            qkv_e[:, t:t + 1024] = dot_t(normed, e_qkv_s[t:t + 1024])

        @pl.when(layer + 1 < layers)
        def _():
            enc_load(0, layer + 1).start()

        for c in range(clips):
            rows = slice(c * slots, (c + 1) * slots)
            for h in range(enc_heads):
                tile = (h * hd_e) // LANES * LANES
                off = h * hd_e - tile
                q_t = roll(qkv_e[rows, tile:tile + LANES], -off)
                k_t = roll(qkv_e[rows, d_enc + tile:d_enc + tile + LANES], -off)
                v_t = roll(qkv_e[rows, 2 * d_enc + tile:2 * d_enc + tile + LANES], hd_e - off)
                qm[c * enc_heads + h] = jnp.where(lane_e < hd_e, q_t, 0.0).astype(BF16)
                kv_t = jnp.where(lane_e < hd_e, k_t, v_t)
                ekvm[c * enc_heads + h] = jnp.where(occupied[c] > 0, kv_t, jnp.inf).astype(BF16)

        kv = ekv.at[layer]

        @pl.when(layer == 0)
        def _():
            pl.semaphore_wait(barrier, chips)

        exchange(layer, ekvm, kv)

        @pl.when(layer == 0)
        def _():
            load_ed.start()
            for copy in dec_loads:
                copy.start()
            load_out.start()

        for c in range(CHUNKS):
            relay(layer, kv, c)
        queries_in(layer)
        for c in range(CHUNKS):
            relayed(layer, kv, c)
        for t in range(0, n, 32):
            block = kv[t:t + 32].reshape(32 * slots, LANES)
            bad = block == jnp.inf
            r = slice(t * slots, (t + 32) * slots)
            clean = jnp.where(bad, jnp.zeros_like(block), block)
            ekvx[r, :LANES] = clean
            ekvx[r, LANES:] = jnp.where(bad & (lane_of(block.shape) == 0), jnp.full_like(block, NEG), jnp.zeros_like(block))
            kvt[:, r] = clean.T
        q = q_in[layer].reshape(m_e, LANES)
        q = jnp.concatenate([q, (lane_of(q.shape) == 0).astype(BF16)], axis=1)
        steps = n_e // bk
        m = jnp.full((1, m_e), NEG, F32)
        l = jnp.zeros((1, m_e), F32)
        acc = jnp.zeros((hd_e, m_e), F32)
        s_buf[0, :, :m_e] = dot_t(ekvx[:bk], q)
        prev = None
        for i in range(steps):
            if i + 1 < steps:
                s_buf[(i + 1) % 2, :, :m_e] = dot_t(ekvx[(i + 1) * bk:(i + 2) * bk], q)
            s = s_buf[i % 2, :, :m_e]
            m_new = jnp.maximum(m, jnp.max(s, axis=0, keepdims=True))
            p = jnp.exp2(s * c_e - m_new * c_e)
            alpha = jnp.exp2((m - m_new) * c_e)
            l = l * alpha + jnp.sum(p, axis=0, keepdims=True)
            p_buf[i % 2, :, :m_e] = p.astype(BF16)
            m = m_new
            if prev is not None:
                j, a = prev
                acc = acc * a + dot(kvt[hd_e:2 * hd_e, j * bk:(j + 1) * bk], p_buf[j % 2, :, :m_e])
            prev = (i, alpha)
        j, a = prev
        acc = acc * a + dot(kvt[hd_e:2 * hd_e, j * bk:(j + 1) * bk], p_buf[j % 2, :, :m_e])
        res = acc / l
        odd = lax.rem(pair, 2) == 1
        zero = jnp.zeros_like(res)
        both = jnp.concatenate([jnp.where(odd, zero, res), jnp.where(odd, res, zero)], axis=0)
        o_s[...] = both.T.astype(BF16).reshape(groups, slots, LANES)

        o_in[layer, pair] = o_s[0]
        for k in range(groups - 1, 0, -1):
            send_home(layer, k // 8, k % 8)
        finish(layer, kv)

        for c in range(clips):
            for g in range(enc_heads // 2):
                first = c * enc_heads + 2 * g
                att_e[c * slots:(c + 1) * slots, g * LANES:(g + 1) * LANES] = (
                    o_in[layer, first].astype(F32) + o_in[layer, first + 1].astype(F32)).astype(BF16)
        enc_load(1, layer).wait()
        mid = (hid_e[...].astype(F32) + dot(att_e[...], e_proj_s[...])).astype(BF16)

        @pl.when(layer + 1 < layers)
        def _():
            enc_load(1, layer + 1).start()

        normed = layer_norm(mid)
        enc_load(2, layer).wait()
        enc_load(3, layer).wait()
        total = mid.astype(F32)
        for t in range(0, e_up_s.shape[1], 1024):
            up = gelu(dot(normed, e_up_s[:, t:t + 1024])).astype(BF16)
            total = total + dot(up, e_down_s[t:t + 1024])

        @pl.when(layer + 1 < layers)
        def _():
            enc_load(2, layer + 1).start()
            enc_load(3, layer + 1).start()

        hid_e[...] = total.astype(BF16)
        return 0

    lax.fori_loop(0, layers, enc_layer, 0)

    load_ed.wait()
    z = dot(layer_norm(hid_e[...]), w_ed_s[...]).astype(BF16)
    for c in range(clips):
        placed = lax.dot_general(selects[c].astype(BF16), z[c * slots:(c + 1) * slots], (((0,), (0,)), ((), ())), preferred_element_type=F32)
        seen = jnp.max(selects[c].T, axis=1, keepdims=True)
        token = jnp.where(seen > 0, placed, mask_token[...].astype(F32))
        hid_d[c * tokens:(c + 1) * tokens] = (token + dec_pos[...].astype(F32)).astype(BF16)

    hd_d = d_dec // dec_heads
    c_d = hd_d ** -0.5 * LOG2E
    half = tokens // 2
    parts = LANES // hd_d
    rows_q = tokens // parts
    n_d = n * half
    q_rows = groups * rows_q
    blk = 128
    m_d = 2 * parts * blk
    h_d = m_d // 2
    per = blk // rows_q
    lane_q = lane_of((rows_q, LANES))
    lane_k = lane_of((half, LANES))
    col = lane_of((LANES, 2 * parts * LANES))
    row = lax.broadcasted_iota(jnp.int32, col.shape, 0)
    part = col // LANES
    inside = lax.rem(col, LANES) - jnp.where(part >= parts, 2 * hd_d, 0)
    pick_s[...] = jnp.where((inside >= 0) & (inside < hd_d) & (row == inside + hd_d * lax.rem(part, parts)), 1.0, 0.0).astype(BF16)
    for copy in dec_loads:
        copy.wait()

    def dec_layer(layer, _):
        phase = layers + layer
        normed = layer_norm(hid_d[...])
        qkv_d[...] = dot_t(normed, d_qkv_s[layer])
        for c in range(clips):
            base = c * tokens
            for h in range(dec_heads):
                tile = (h * hd_d) // LANES * LANES
                off = h * hd_d - tile
                lo = slice(base, base + half)
                hi = slice(base + half, base + tokens)
                kc = slice(d_dec + tile, d_dec + tile + LANES)
                vc = slice(2 * d_dec + tile, 2 * d_dec + tile + LANES)
                k_lo, v_lo = roll(qkv_d[lo, kc], -off), roll(qkv_d[lo, vc], hd_d - off)
                k_hi, v_hi = roll(qkv_d[hi, kc], 2 * hd_d - off), roll(qkv_d[hi, vc], 3 * hd_d - off)
                dkvm[c * dec_heads + h] = jnp.where(
                    lane_k < 2 * hd_d, jnp.where(lane_k < hd_d, k_lo, v_lo), jnp.where(lane_k < 3 * hd_d, k_hi, v_hi)).astype(BF16)
                packed = None
                for j in range(parts):
                    moved = roll(qkv_d[base + j * rows_q:base + (j + 1) * rows_q, tile:tile + LANES], hd_d * j - off)
                    packed = moved if packed is None else jnp.where(lane_q >= hd_d * j, moved, packed)
                qm[c * dec_heads + h] = packed.astype(BF16)
        kv = dkv.at[layer]
        exchange(phase, dkvm, kv)
        relay(phase, kv, 0)
        queries_in(phase)
        spread = dot(q_in[phase].reshape(q_rows, LANES), pick_s[...])
        for b in range(q_rows // blk):
            for t in range(2 * parts):
                qq[b * m_d + t * blk:b * m_d + (t + 1) * blk] = spread[b * blk:(b + 1) * blk, t * LANES:(t + 1) * LANES].astype(BF16)

        msgs = bk // half
        blocks = q_rows // blk
        steps = 2 * per_chunk // msgs
        direct = per_chunk // msgs

        def scores(block, message, slot):
            q = qq[pl.ds(pl.multiple_of(block * m_d, m_d), m_d)]
            s_buf[slot] = dot_t(kv[pl.ds(message, msgs)].reshape(bk, LANES), q)

        for c in range(CHUNKS):
            if c + 1 < CHUNKS:
                relay(phase, kv, c + 1)
            relayed(phase, kv, c)
            places = [c * per_chunk + i * msgs for i in range(direct)] + [chips + c * per_chunk + i * msgs for i in range(steps - direct)]
            for t in places:
                kvt[:, t * half:t * half + bk] = kv[t:t + msgs].reshape(bk, LANES).T
            if c == 0:
                scores(blocks - 1, 0, 0)

            def q_block(b, _):
                block = blocks - 1 - b
                if c == 0:
                    m = jnp.full((1, m_d), NEG, F32)
                    l = jnp.zeros((1, m_d), F32)
                    acc_a = jnp.zeros((hd_d, h_d), F32)
                    acc_b = jnp.zeros((hd_d, h_d), F32)
                else:
                    m, l, acc_a, acc_b = m_st[block], l_st[block], acc_st[block, 0], acc_st[block, 1]
                alphas = []

                def add(i, acc_a, acc_b):
                    keys = slice(places[i] * half, places[i] * half + bk)
                    acc_a = acc_a * alphas[i][:, :h_d] + dot(kvt[hd_d:2 * hd_d, keys], p_buf[i % 2, :, :h_d])
                    acc_b = acc_b * alphas[i][:, h_d:] + dot(kvt[3 * hd_d:4 * hd_d, keys], p_buf[i % 2, :, h_d:])
                    return acc_a, acc_b

                for i in range(steps):
                    if i + 1 < steps:
                        scores(block, places[i + 1], (i + 1) % 2)
                    else:
                        ahead = min(c + 1, CHUNKS - 1) - c
                        last = b // (blocks - 1)
                        scores(lax.rem(block + blocks - 1, blocks), (c + ahead * last) * per_chunk, 0)
                    s = s_buf[i % 2]
                    m_new = jnp.maximum(m, jnp.max(s, axis=0, keepdims=True))
                    p = jnp.exp2(s * c_d - m_new * c_d)
                    alphas.append(jnp.exp2((m - m_new) * c_d))
                    l = l * alphas[i] + jnp.sum(p, axis=0, keepdims=True)
                    p_buf[i % 2] = p.astype(BF16)
                    m = m_new
                    if i > 0:
                        acc_a, acc_b = add(i - 1, acc_a, acc_b)
                acc_a, acc_b = add(steps - 1, acc_a, acc_b)
                if c + 1 < CHUNKS:
                    m_st[block], l_st[block], acc_st[block, 0], acc_st[block, 1] = m, l, acc_a, acc_b
                    return 0
                m_all = jnp.maximum(m[:, :h_d], m[:, h_d:])
                e_a = jnp.exp2((m[:, :h_d] - m_all) * c_d)
                e_b = jnp.exp2((m[:, h_d:] - m_all) * c_d)
                res = (acc_a * e_a + acc_b * e_b) / (l[:, :h_d] * e_a + l[:, h_d:] * e_b)
                stacked = jnp.concatenate([res[:, j * blk:(j + 1) * blk] for j in range(parts)], axis=0)
                o_s[pl.ds(block * per, per)] = stacked.T.astype(BF16).reshape(per, rows_q, LANES)
                for j in range(1, per):
                    send_home(phase, block, j)

                @pl.when(block > 0)
                def _():
                    send_home(phase, block, 0)
                return 0

            lax.fori_loop(0, blocks, q_block, 0)
        o_in[phase, pair] = o_s[0]
        finish(phase, kv)

        for c in range(clips):
            for g in range(dec_heads // parts):
                got = [o_in[phase, c * dec_heads + parts * g + h].astype(F32) for h in range(parts)]
                for j in range(parts):
                    tile = None
                    for h in range(parts):
                        moved = roll(got[h], hd_d * (h - j))
                        tile = moved if tile is None else jnp.where(lane_q >= hd_d * h, moved, tile)
                    att_d[c * tokens + j * rows_q:c * tokens + (j + 1) * rows_q, g * LANES:(g + 1) * LANES] = tile.astype(BF16)
        mid = (hid_d[...].astype(F32) + dot(att_d[...], d_proj_s[layer])).astype(BF16)
        up = gelu(dot(layer_norm(mid), d_up_s[layer])).astype(BF16)
        hid_d[...] = (mid.astype(F32) + dot(up, d_down_s[layer])).astype(BF16)
        return 0

    lax.fori_loop(0, layers, dec_layer, 0)
    load_out.wait()
    result = dot(layer_norm(hid_d[...]), w_out_s[...])
    for c in range(clips):
        out[c] = result[c * tokens:(c + 1) * tokens]


def solution(mesh):
    n = mesh.shape['sp']

    def local_program(patches, vis_mask, enc_pos, dec_pos, w_pe, b_pe, enc_qkv, enc_proj, enc_up, enc_down, w_ed, mask_token, dec_qkv, dec_proj, dec_up, dec_down, w_out):
        clips, tokens, width = patches.shape
        layers, d_enc, _, enc_heads, _ = enc_qkv.shape
        _, d_dec, _, dec_heads, _ = dec_qkv.shape
        slots = 2 * (tokens // KEEP_DIV)
        half = tokens // 2
        groups = n // QUARTERS
        f_enc, f_dec = enc_up.shape[2], dec_up.shape[2]
        e_rows, d_rows = clips * slots, clips * tokens
        phases = 2 * layers
        bk, m_d = 256, 1024
        vmem = pl.BlockSpec(memory_space=pltpu.VMEM)
        hbm = pl.BlockSpec(memory_space=pl.ANY)

        def buf(*shape, dtype=BF16):
            return pltpu.VMEM(shape, dtype)

        def sems(*shape):
            return pltpu.SemaphoreType.DMA(shape)

        return pl.pallas_call(
            functools.partial(model_kernel, n, enc_heads, dec_heads),
            out_shape=jax.ShapeDtypeStruct((clips, tokens, w_out.shape[1]), F32),
            in_specs=[vmem] * 6 + [hbm] * 11,
            out_specs=vmem,
            scratch_shapes=[
                buf(width, d_enc), buf(3 * d_enc, d_enc), buf(d_enc, d_enc), buf(d_enc, f_enc), buf(f_enc, d_enc), buf(d_enc, d_dec),
                buf(layers, 3 * d_dec, d_dec), buf(layers, d_dec, d_dec), buf(layers, d_dec, f_dec), buf(layers, f_dec, d_dec), buf(d_dec, w_out.shape[1]),
                buf(groups, slots, LANES), buf(groups, half, LANES), buf(groups, MSG, LANES), buf(groups, MSG, LANES),
                buf(layers, n, slots, LANES), buf(layers, n, half, LANES), buf(phases, groups, MSG, LANES), buf(phases, groups, MSG, LANES),
                buf(n * slots, 2 * LANES), buf(LANES, n * half), buf(groups * MSG * 8, LANES),
                buf(2, bk, m_d, dtype=F32), buf(2, bk, m_d),
                buf(e_rows, d_enc), buf(e_rows, 3 * d_enc, dtype=F32), buf(e_rows, d_enc),
                buf(d_rows, d_dec), buf(d_rows, 3 * d_dec, dtype=F32), buf(d_rows, d_dec),
                buf(LANES, 8 * LANES),
                buf(4, 1, m_d, dtype=F32), buf(4, 1, m_d, dtype=F32), buf(4, 2, LANES // 4, m_d // 2, dtype=F32),
                pltpu.SemaphoreType.DMA((11,)),
                sems(phases), sems(phases, CHUNKS), sems(phases), sems(phases, CHUNKS), sems(phases), sems(phases), sems(phases), sems(phases),
            ],
            compiler_params=pltpu.CompilerParams(collective_id=0, has_side_effects=True, vmem_limit_bytes=67043328),
            name='model',
        )(patches, vis_mask, enc_pos, dec_pos, b_pe.reshape(1, -1), mask_token.reshape(1, -1), w_pe,
          enc_qkv.transpose(0, 2, 3, 4, 1).reshape(layers, 3 * d_enc, d_enc), enc_proj.reshape(layers, d_enc, d_enc), enc_up, enc_down, w_ed,
          dec_qkv.transpose(0, 2, 3, 4, 1).reshape(layers, 3 * d_dec, d_dec), dec_proj.reshape(layers, d_dec, d_dec), dec_up, dec_down, w_out)

    row_spec = P('dp', 'sp', None)
    pos_spec = P(('dp', 'sp'), None)
    arg_specs = (row_spec, P('dp', 'sp'), pos_spec, pos_spec) + (P(),) * 13
    return jax.shard_map(local_program, mesh=mesh, in_specs=arg_specs, out_specs=row_spec, check_vma=False)
```

```python
import functools

import jax
import jax.numpy as jnp
from jax import lax
from jax.experimental import pallas as pl
from jax.experimental.pallas import tpu as pltpu
from jax.sharding import PartitionSpec as P

KEEP_DIV = 8
LANES = 128
QUARTERS = 4
MSG = 16
LOG2E = 1.4426950408889634
NEG = -3e38
SIDE = 4
CHUNKS = 4
BF16 = jnp.bfloat16
F32 = jnp.float32


def layer_norm(hidden):
    hid_f32 = hidden.astype(F32)
    centred = hid_f32 - jnp.mean(hid_f32, axis=-1, keepdims=True)
    row_var = jnp.mean(centred * centred, axis=-1, keepdims=True)
    return (centred * lax.rsqrt(row_var + 1e-6)).astype(BF16)


def gelu(x):
    return 0.5 * x * (1.0 + lax.erf(x * (0.5 ** 0.5)))


def dot(a, b):
    return jnp.dot(a, b, preferred_element_type=F32)


def dot_t(a, b):
    return lax.dot_general(a, b, (((1,), (1,)), ((), ())), preferred_element_type=F32)


def lane_of(shape):
    return lax.broadcasted_iota(jnp.int32, shape, len(shape) - 1)


def roll(x, shift):
    shift = shift % LANES
    return x if shift == 0 else pltpu.roll(x, shift, 1)


def row_of(ref):
    rows = ref[...].astype(F32)
    return jnp.concatenate([rows[i:i + 1] for i in range(rows.shape[0])], axis=1)


def wait_bytes(ref, sem):
    pltpu.make_async_copy(ref, ref, sem).wait()


def model_kernel(n, enc_heads, dec_heads, mask, b_pe, mask_token, patches_h, enc_pos_h, dec_pos_h,
                 w_pe, e_qkv, e_proj, e_up, e_down, w_ed, d_qkv, d_proj, d_up, d_down, w_out, out,
                 patches, enc_pos, dec_pos, w_pe_s, e_qkv_s, e_proj_s, e_up_s, e_down_s, w_ed_s, d_qkv_s, d_proj_s, d_up_s, d_down_s, w_out_s,
                 ekvm, dkvm, qm, o_s, ekv, dkv, q_in, o_in, ekvx, kvt, qq, s_buf, p_buf, hid_e, qkv_e, att_e, hid_d, qkv_d, att_d, pick_s,
                 m_st, l_st, acc_st, wsem, kv_send, kv_recv, f_send, f_recv, q_send, q_recv, o_send, o_recv):
    me = lax.axis_index('sp')
    groups = n // QUARTERS
    pair = me // QUARTERS
    chips = n // 2
    per_chunk = chips // CHUNKS
    core = lax.rem(me, 2)
    partner = me + 1 - 2 * core
    at_z, at_y, at_x = me // 32, lax.rem(me // 8, SIDE), lax.rem(me // 2, SIDE)

    def device_at(dz, dy, dx):
        return (lax.rem(at_z + dz, SIDE) * SIDE + lax.rem(at_y + dy, SIDE)) * 8 + lax.rem(at_x + dx, SIDE) * 2 + core

    far = {0: 0, 1: 1, 2: 2, 3: 1}
    offsets = sorted(((dz, dy, dx) for dz in range(SIDE) for dy in range(SIDE) for dx in range(SIDE)), key=lambda o: far[o[0]] + far[o[1]] + far[o[2]])

    def query_offset(block, j):
        return 2 * lax.rem(block, 2) + j // 4, j % 4, 2 * (block // 2)

    def back(d):
        return SIDE - d
    clips, tokens, _ = patches.shape
    slots = 2 * (tokens // KEEP_DIV)
    layers = e_qkv.shape[0]
    d_enc = enc_pos.shape[1]
    d_dec = dec_pos.shape[1]
    mesh_id = pl.DeviceIdType.MESH

    def load(src, dst, i):
        return pltpu.make_async_copy(src, dst, wsem.at[i])

    load_pe = load(w_pe, w_pe_s, 0)
    load_ed = load(w_ed, w_ed_s, 5)
    load_out = load(w_out, w_out_s, 10)
    enc_loads = [(e_qkv, e_qkv_s, 1), (e_proj, e_proj_s, 2), (e_up, e_up_s, 3), (e_down, e_down_s, 4)]
    dec_loads = [load(d_qkv, d_qkv_s, 6), load(d_proj, d_proj_s, 7), load(d_up, d_up_s, 8), load(d_down, d_down_s, 9)]

    def enc_load(which, layer):
        src, dst, i = enc_loads[which]
        return load(src.at[layer], dst, i)

    first_loads = [load(patches_h, patches, 11), load(enc_pos_h, enc_pos, 12), load(dec_pos_h, dec_pos, 13)]
    for copy in first_loads:
        copy.start()
    load_pe.start()
    enc_load(0, 0).start()

    barrier = pltpu.get_barrier_semaphore()

    def greet(i, _):
        pl.semaphore_signal(barrier, inc=1, device_id={'sp': lax.rem(me + 2 * i, n)}, device_id_type=mesh_id)
        return 0

    lax.fori_loop(1, chips, greet, 0)
    pl.semaphore_signal(barrier, inc=1, device_id={'sp': partner}, device_id_type=mesh_id)

    mask_f = mask[...].astype(F32)
    before = lax.broadcasted_iota(jnp.int32, (tokens, tokens), 0) < lax.broadcasted_iota(jnp.int32, (tokens, tokens), 1)
    rank = dot(mask_f.astype(BF16), before.astype(BF16))
    slot_id = lax.broadcasted_iota(jnp.int32, (slots, tokens), 0).astype(F32)
    selects, moved_x, moved_pos, occupied = [], [], [], []
    for copy in first_loads:
        copy.wait()
    for c in range(clips):
        select = jnp.where((rank[c:c + 1] == slot_id) & (mask_f[c:c + 1] > 0), 1.0, 0.0)
        selects.append(select)
        moved_x.append(dot(select.astype(BF16), patches[c]).astype(BF16))
        moved_pos.append(dot(select.astype(BF16), enc_pos[...]))
        occupied.append(jnp.sum(select, axis=1, keepdims=True))
    load_pe.wait()
    embedded = dot(jnp.concatenate(moved_x, axis=0), w_pe_s[...]) + row_of(b_pe) + jnp.concatenate(moved_pos, axis=0)
    hid_e[...] = embedded.astype(BF16)
    for which in range(1, 4):
        enc_load(which, 0).start()

    def send_kv(phase, kvm, kv, order):
        for i in order:
            to = device_at(*offsets[i])
            pltpu.make_async_remote_copy(
                src_ref=kvm.at[to // QUARTERS], dst_ref=kv.at[i], send_sem=kv_send.at[phase], recv_sem=kv_recv.at[phase, i // per_chunk],
                device_id={'sp': to}, device_id_type=mesh_id).start()

    def send_q(phase, order):
        for k in order:
            to = device_at(*query_offset(k // 8, k % 8))
            pltpu.make_async_remote_copy(
                src_ref=qm.at[to // QUARTERS], dst_ref=q_in.at[phase, k], send_sem=q_send.at[phase], recv_sem=q_recv.at[phase, k // 8],
                device_id={'sp': to}, device_id_type=mesh_id).start()

    def relay(phase, kv, c):
        first = 1 if isinstance(c, int) and c == 0 else 0
        wait_bytes(kv.at[pl.ds(c * per_chunk + first, per_chunk - first)], kv_recv.at[phase, c])
        pltpu.make_async_remote_copy(
            src_ref=kv.at[pl.ds(c * per_chunk, per_chunk)], dst_ref=kv.at[pl.ds(chips + c * per_chunk, per_chunk)],
            send_sem=f_send.at[phase], recv_sem=f_recv.at[phase, c], device_id={'sp': partner}, device_id_type=mesh_id).start()

    def relayed(phase, kv, c):
        wait_bytes(kv.at[pl.ds(chips + c * per_chunk, per_chunk)], f_recv.at[phase, c])

    def queries_in(phase, block):
        first = 1 if isinstance(block, int) and block == 0 else 0
        wait_bytes(q_in.at[phase, pl.ds(8 * block + first, 8 - first)], q_recv.at[phase, block])

    def send_home(phase, block, j):
        dz, dy, dx = query_offset(block, j)
        to = device_at(back(dz), back(dy), back(dx))
        pltpu.make_async_remote_copy(
            src_ref=o_s.at[8 * block + j], dst_ref=o_in.at[phase, pair], send_sem=o_send.at[phase], recv_sem=o_recv.at[phase],
            device_id={'sp': to}, device_id_type=mesh_id).start()

    def finish(phase, kv):
        rest = pl.ds(1, groups - 1)
        wait_bytes(o_in.at[phase, rest], o_recv.at[phase])
        wait_bytes(o_s.at[rest], o_send.at[phase])
        wait_bytes(qm.at[rest], q_send.at[phase])
        wait_bytes(kv.at[pl.ds(1, chips - 1)], kv_send.at[phase])
        wait_bytes(kv.at[pl.ds(0, chips)], f_send.at[phase])

    hd_e = d_enc // enc_heads
    lane_e = lane_of((slots, LANES))
    c_e = hd_e ** -0.5 * LOG2E
    n_e = n * slots
    m_e = groups * slots
    bk = 256

    def enc_layer(layer, _):
        normed = layer_norm(hid_e[...])
        enc_load(0, layer).wait()
        for t in range(d_enc, 3 * d_enc, 1024):
            qkv_e[:, t:t + 1024] = dot_t(normed, e_qkv_s[t:t + 1024])

        for c in range(clips):
            rows = slice(c * slots, (c + 1) * slots)
            for h in range(enc_heads):
                tile = (h * hd_e) // LANES * LANES
                off = h * hd_e - tile
                k_t = roll(qkv_e[rows, d_enc + tile:d_enc + tile + LANES], -off)
                v_t = roll(qkv_e[rows, 2 * d_enc + tile:2 * d_enc + tile + LANES], hd_e - off)
                kv_t = jnp.where(lane_e < hd_e, k_t, v_t)
                ekvm[c * enc_heads + h] = jnp.where(occupied[c] > 0, kv_t, jnp.inf).astype(BF16)

        kv = ekv.at[layer]

        @pl.when(layer == 0)
        def _():
            pl.semaphore_wait(barrier, chips)

        send_kv(layer, ekvm, kv, range(chips - 1, 0, -1))
        qkv_e[:, :d_enc] = dot_t(normed, e_qkv_s[:d_enc])
        for c in range(clips):
            rows = slice(c * slots, (c + 1) * slots)
            for h in range(enc_heads):
                tile = (h * hd_e) // LANES * LANES
                q_t = roll(qkv_e[rows, tile:tile + LANES], tile - h * hd_e)
                qm[c * enc_heads + h] = jnp.where(lane_e < hd_e, q_t, 0.0).astype(BF16)
        send_q(layer, range(groups - 1, 0, -1))
        q_in[layer, 0] = qm[pair]
        kv[0] = ekvm[pair]

        @pl.when(layer + 1 < layers)
        def _():
            enc_load(0, layer + 1).start()

        @pl.when(layer == 0)
        def _():
            load_ed.start()
            for copy in dec_loads:
                copy.start()
            load_out.start()

        for c in (2, 1, 0, 3):
            relay(layer, kv, c)
        for block in range(4):
            queries_in(layer, block)
        for c in (2, 1, 0, 3):
            relayed(layer, kv, c)
        for t in range(0, n, 32):
            block = kv[t:t + 32].reshape(32 * slots, LANES)
            bad = block == jnp.inf
            r = slice(t * slots, (t + 32) * slots)
            clean = jnp.where(bad, jnp.zeros_like(block), block)
            ekvx[r, :LANES] = clean
            ekvx[r, LANES:] = jnp.where(bad & (lane_of(block.shape) == 0), jnp.full_like(block, NEG), jnp.zeros_like(block))
            kvt[:, r] = clean.T
        q = q_in[layer].reshape(m_e, LANES)
        q = jnp.concatenate([q, (lane_of(q.shape) == 0).astype(BF16)], axis=1)
        steps = n_e // bk
        m = jnp.full((1, m_e), NEG, F32)
        l = jnp.zeros((1, m_e), F32)
        acc = jnp.zeros((hd_e, m_e), F32)
        s_buf[0, :, :m_e] = dot_t(ekvx[:bk], q)
        prev = None
        for i in range(steps):
            if i + 1 < steps:
                s_buf[(i + 1) % 2, :, :m_e] = dot_t(ekvx[(i + 1) * bk:(i + 2) * bk], q)
            s = s_buf[i % 2, :, :m_e]
            m_new = jnp.maximum(m, jnp.max(s, axis=0, keepdims=True))
            p = jnp.exp2(s * c_e - m_new * c_e)
            alpha = jnp.exp2((m - m_new) * c_e)
            l = l * alpha + jnp.sum(p, axis=0, keepdims=True)
            p_buf[i % 2, :, :m_e] = p.astype(BF16)
            m = m_new
            if prev is not None:
                j, a = prev
                acc = acc * a + dot(kvt[hd_e:2 * hd_e, j * bk:(j + 1) * bk], p_buf[j % 2, :, :m_e])
            prev = (i, alpha)
        j, a = prev
        acc = acc * a + dot(kvt[hd_e:2 * hd_e, j * bk:(j + 1) * bk], p_buf[j % 2, :, :m_e])
        res = acc / l
        odd = lax.rem(pair, 2) == 1
        zero = jnp.zeros_like(res)
        both = jnp.concatenate([jnp.where(odd, zero, res), jnp.where(odd, res, zero)], axis=0)
        o_s[...] = both.T.astype(BF16).reshape(groups, slots, LANES)

        o_in[layer, pair] = o_s[0]
        for k in range(groups - 1, 0, -1):
            send_home(layer, k // 8, k % 8)
        finish(layer, kv)

        for c in range(clips):
            for g in range(enc_heads // 2):
                first = c * enc_heads + 2 * g
                att_e[c * slots:(c + 1) * slots, g * LANES:(g + 1) * LANES] = (
                    o_in[layer, first].astype(F32) + o_in[layer, first + 1].astype(F32)).astype(BF16)
        enc_load(1, layer).wait()
        mid = (hid_e[...].astype(F32) + dot(att_e[...], e_proj_s[...])).astype(BF16)

        @pl.when(layer + 1 < layers)
        def _():
            enc_load(1, layer + 1).start()

        normed = layer_norm(mid)
        enc_load(2, layer).wait()
        enc_load(3, layer).wait()
        total = mid.astype(F32)
        for t in range(0, e_up_s.shape[1], 1024):
            up = gelu(dot(normed, e_up_s[:, t:t + 1024])).astype(BF16)
            total = total + dot(up, e_down_s[t:t + 1024])

        @pl.when(layer + 1 < layers)
        def _():
            enc_load(2, layer + 1).start()
            enc_load(3, layer + 1).start()

        hid_e[...] = total.astype(BF16)
        return 0

    lax.fori_loop(0, layers, enc_layer, 0)

    load_ed.wait()
    z = dot(layer_norm(hid_e[...]), w_ed_s[...]).astype(BF16)
    for c in range(clips):
        placed = lax.dot_general(selects[c].astype(BF16), z[c * slots:(c + 1) * slots], (((0,), (0,)), ((), ())), preferred_element_type=F32)
        seen = jnp.max(selects[c].T, axis=1, keepdims=True)
        token = jnp.where(seen > 0, placed, row_of(mask_token))
        hid_d[c * tokens:(c + 1) * tokens] = (token + dec_pos[...].astype(F32)).astype(BF16)

    hd_d = d_dec // dec_heads
    c_d = hd_d ** -0.5 * LOG2E
    half = tokens // 2
    parts = LANES // hd_d
    rows_q = tokens // parts
    n_d = n * half
    q_rows = groups * rows_q
    blk = 128
    m_d = 2 * parts * blk
    h_d = m_d // 2
    per = blk // rows_q
    lane_q = lane_of((rows_q, LANES))
    lane_k = lane_of((half, LANES))
    col = lane_of((LANES, 2 * parts * LANES))
    row = lax.broadcasted_iota(jnp.int32, col.shape, 0)
    part = col // LANES
    inside = lax.rem(col, LANES) - jnp.where(part >= parts, 2 * hd_d, 0)
    pick_s[...] = jnp.where((inside >= 0) & (inside < hd_d) & (row == inside + hd_d * lax.rem(part, parts)), 1.0, 0.0).astype(BF16)
    for copy in dec_loads:
        copy.wait()

    def dec_layer(layer, _):
        phase = layers + layer
        normed = layer_norm(hid_d[...])
        kv = dkv.at[layer]
        qkv_d[:, d_dec:] = dot_t(normed, d_qkv_s[layer, d_dec:])
        for c in range(clips):
            base = c * tokens
            for h in range(dec_heads):
                tile = (h * hd_d) // LANES * LANES
                off = h * hd_d - tile
                lo = slice(base, base + half)
                hi = slice(base + half, base + tokens)
                kc = slice(d_dec + tile, d_dec + tile + LANES)
                vc = slice(2 * d_dec + tile, 2 * d_dec + tile + LANES)
                k_lo, v_lo = roll(qkv_d[lo, kc], -off), roll(qkv_d[lo, vc], hd_d - off)
                k_hi, v_hi = roll(qkv_d[hi, kc], 2 * hd_d - off), roll(qkv_d[hi, vc], 3 * hd_d - off)
                dkvm[c * dec_heads + h] = jnp.where(
                    lane_k < 2 * hd_d, jnp.where(lane_k < hd_d, k_lo, v_lo), jnp.where(lane_k < 3 * hd_d, k_hi, v_hi)).astype(BF16)
        send_kv(phase, dkvm, kv, range(1, per_chunk))
        qkv_d[:, :d_dec] = dot_t(normed, d_qkv_s[layer, :d_dec])
        for c in range(clips):
            base = c * tokens
            for h in range(dec_heads):
                tile = (h * hd_d) // LANES * LANES
                off = h * hd_d - tile
                packed = None
                for j in range(parts):
                    moved = roll(qkv_d[base + j * rows_q:base + (j + 1) * rows_q, tile:tile + LANES], hd_d * j - off)
                    packed = moved if packed is None else jnp.where(lane_q >= hd_d * j, moved, packed)
                qm[c * dec_heads + h] = packed.astype(BF16)
        send_q(phase, range(1, groups))
        send_kv(phase, dkvm, kv, range(per_chunk, chips))
        q_in[phase, 0] = qm[pair]
        kv[0] = dkvm[pair]

        msgs = bk // half
        blocks = q_rows // blk

        def spread(block):
            queries_in(phase, block)
            wide = dot(q_in[phase, pl.ds(8 * block, 8)].reshape(blk, LANES), pick_s[...])
            for t in range(2 * parts):
                qq[pl.ds(pl.multiple_of(block * m_d + t * blk, blk), blk)] = wide[:, t * LANES:(t + 1) * LANES].astype(BF16)

        def transpose(places):
            for t in places:
                kvt[:, t * half:t * half + bk] = kv[t:t + msgs].reshape(bk, LANES).T

        def scores(block, message, slot):
            q = qq[pl.ds(pl.multiple_of(block * m_d, m_d), m_d)]
            s_buf[slot] = dot_t(kv[pl.ds(message, msgs)].reshape(bk, LANES), q)

        def attend(block, places, state, next_block, next_message):
            m, l, acc_a, acc_b = state
            alphas = []
            steps = len(places)

            def add(i, acc_a, acc_b):
                keys = slice(places[i] * half, places[i] * half + bk)
                acc_a = acc_a * alphas[i][:, :h_d] + dot(kvt[hd_d:2 * hd_d, keys], p_buf[i % 2, :, :h_d])
                acc_b = acc_b * alphas[i][:, h_d:] + dot(kvt[3 * hd_d:4 * hd_d, keys], p_buf[i % 2, :, h_d:])
                return acc_a, acc_b

            for i in range(steps):
                if i + 1 < steps:
                    scores(block, places[i + 1], (i + 1) % 2)
                else:
                    scores(next_block, next_message, 0)
                s = s_buf[i % 2]
                m_new = jnp.maximum(m, jnp.max(s, axis=0, keepdims=True))
                p = jnp.exp2(s * c_d - m_new * c_d)
                alphas.append(jnp.exp2((m - m_new) * c_d))
                l = l * alphas[i] + jnp.sum(p, axis=0, keepdims=True)
                p_buf[i % 2] = p.astype(BF16)
                m = m_new
                if i > 0:
                    acc_a, acc_b = add(i - 1, acc_a, acc_b)
            acc_a, acc_b = add(steps - 1, acc_a, acc_b)
            return m, l, acc_a, acc_b

        near = [i for i in range(0, per_chunk, msgs)]
        near = near + [chips + i for i in near]
        rest = [i for i in range(per_chunk, chips, msgs)]
        rest = rest + [chips + i for i in rest]

        relay(phase, kv, 0)
        spread(0)
        spread(1)
        relayed(phase, kv, 0)
        transpose(near)
        scores(0, near[0], 0)

        def near_block(b, _):
            @pl.when(b > 0)
            def _():
                relay(phase, kv, b)

            @pl.when(b + 2 < blocks)
            def _():
                spread(b + 2)

            fresh = (jnp.full((1, m_d), NEG, F32), jnp.zeros((1, m_d), F32), jnp.zeros((hd_d, h_d), F32), jnp.zeros((hd_d, h_d), F32))
            state = attend(b, near, fresh, jnp.minimum(b + 1, blocks - 1), near[0] + (b // (blocks - 1)) * (rest[0] - near[0]))
            m_st[b], l_st[b], acc_st[b, 0], acc_st[b, 1] = state
            return 0

        lax.fori_loop(0, blocks, near_block, 0)
        for c in range(1, CHUNKS):
            relayed(phase, kv, c)
        transpose(rest)

        def rest_block(b, _):
            block = blocks - 1 - b
            state = (m_st[block], l_st[block], acc_st[block, 0], acc_st[block, 1])
            m, l, acc_a, acc_b = attend(block, rest, state, lax.rem(block + blocks - 1, blocks), rest[0])
            m_all = jnp.maximum(m[:, :h_d], m[:, h_d:])
            e_a = jnp.exp2((m[:, :h_d] - m_all) * c_d)
            e_b = jnp.exp2((m[:, h_d:] - m_all) * c_d)
            res = (acc_a * e_a + acc_b * e_b) / (l[:, :h_d] * e_a + l[:, h_d:] * e_b)
            stacked = jnp.concatenate([res[:, j * blk:(j + 1) * blk] for j in range(parts)], axis=0)
            o_s[pl.ds(block * per, per)] = stacked.T.astype(BF16).reshape(per, rows_q, LANES)
            for j in range(1, per):
                send_home(phase, block, j)

            @pl.when(block > 0)
            def _():
                send_home(phase, block, 0)
            return 0

        lax.fori_loop(0, blocks, rest_block, 0)
        o_in[phase, pair] = o_s[0]
        finish(phase, kv)

        for c in range(clips):
            for g in range(dec_heads // parts):
                got = [o_in[phase, c * dec_heads + parts * g + h].astype(F32) for h in range(parts)]
                for j in range(parts):
                    tile = None
                    for h in range(parts):
                        moved = roll(got[h], hd_d * (h - j))
                        tile = moved if tile is None else jnp.where(lane_q >= hd_d * h, moved, tile)
                    att_d[c * tokens + j * rows_q:c * tokens + (j + 1) * rows_q, g * LANES:(g + 1) * LANES] = tile.astype(BF16)
        mid = (hid_d[...].astype(F32) + dot(att_d[...], d_proj_s[layer])).astype(BF16)
        up = gelu(dot(layer_norm(mid), d_up_s[layer])).astype(BF16)
        hid_d[...] = (mid.astype(F32) + dot(up, d_down_s[layer])).astype(BF16)
        return 0

    lax.fori_loop(0, layers, dec_layer, 0)
    load_out.wait()
    result = dot(layer_norm(hid_d[...]), w_out_s[...])
    for c in range(clips):
        out[c] = result[c * tokens:(c + 1) * tokens]


def solution(mesh):
    n = mesh.shape['sp']

    def local_program(patches, vis_mask, enc_pos, dec_pos, w_pe, b_pe, enc_qkv, enc_proj, enc_up, enc_down, w_ed, mask_token, dec_qkv, dec_proj, dec_up, dec_down, w_out):
        clips, tokens, width = patches.shape
        layers, d_enc, _, enc_heads, _ = enc_qkv.shape
        _, d_dec, _, dec_heads, _ = dec_qkv.shape
        slots = 2 * (tokens // KEEP_DIV)
        half = tokens // 2
        groups = n // QUARTERS
        f_enc, f_dec = enc_up.shape[2], dec_up.shape[2]
        e_rows, d_rows = clips * slots, clips * tokens
        phases = 2 * layers
        bk, m_d = 256, 1024
        vmem = pl.BlockSpec(memory_space=pltpu.VMEM)
        hbm = pl.BlockSpec(memory_space=pl.ANY)

        def buf(*shape, dtype=BF16):
            return pltpu.VMEM(shape, dtype)

        def sems(*shape):
            return pltpu.SemaphoreType.DMA(shape)

        return pl.pallas_call(
            functools.partial(model_kernel, n, enc_heads, dec_heads),
            out_shape=jax.ShapeDtypeStruct((clips, tokens, w_out.shape[1]), F32),
            in_specs=[vmem] * 3 + [hbm] * 14,
            out_specs=vmem,
            scratch_shapes=[
                buf(clips, tokens, width), buf(tokens, d_enc), buf(tokens, d_dec),
                buf(width, d_enc), buf(3 * d_enc, d_enc), buf(d_enc, d_enc), buf(d_enc, f_enc), buf(f_enc, d_enc), buf(d_enc, d_dec),
                buf(layers, 3 * d_dec, d_dec), buf(layers, d_dec, d_dec), buf(layers, d_dec, f_dec), buf(layers, f_dec, d_dec), buf(d_dec, w_out.shape[1]),
                buf(groups, slots, LANES), buf(groups, half, LANES), buf(groups, MSG, LANES), buf(groups, MSG, LANES),
                buf(layers, n, slots, LANES), buf(layers, n, half, LANES), buf(phases, groups, MSG, LANES), buf(phases, groups, MSG, LANES),
                buf(n * slots, 2 * LANES), buf(LANES, n * half), buf(groups * MSG * 8, LANES),
                buf(2, bk, m_d, dtype=F32), buf(2, bk, m_d),
                buf(e_rows, d_enc), buf(e_rows, 3 * d_enc, dtype=F32), buf(e_rows, d_enc),
                buf(d_rows, d_dec), buf(d_rows, 3 * d_dec, dtype=F32), buf(d_rows, d_dec),
                buf(LANES, 8 * LANES),
                buf(4, 1, m_d, dtype=F32), buf(4, 1, m_d, dtype=F32), buf(4, 2, LANES // 4, m_d // 2, dtype=F32),
                pltpu.SemaphoreType.DMA((14,)),
                sems(phases), sems(phases, CHUNKS), sems(phases), sems(phases, CHUNKS), sems(phases), sems(phases, 4), sems(phases), sems(phases),
            ],
            compiler_params=pltpu.CompilerParams(collective_id=0, has_side_effects=True, vmem_limit_bytes=67043328),
            name='model',
        )(vis_mask, b_pe.reshape(-1, LANES), mask_token.reshape(-1, LANES), patches, enc_pos, dec_pos, w_pe,
          enc_qkv.transpose(0, 2, 3, 4, 1).reshape(layers, 3 * d_enc, d_enc), enc_proj.reshape(layers, d_enc, d_enc), enc_up, enc_down, w_ed,
          dec_qkv.transpose(0, 2, 3, 4, 1).reshape(layers, 3 * d_dec, d_dec), dec_proj.reshape(layers, d_dec, d_dec), dec_up, dec_down, w_out)

    row_spec = P('dp', 'sp', None)
    pos_spec = P(('dp', 'sp'), None)
    arg_specs = (row_spec, P('dp', 'sp'), pos_spec, pos_spec) + (P(),) * 13
    return jax.shard_map(local_program, mesh=mesh, in_specs=arg_specs, out_specs=row_spec, check_vma=False)
```

```python
import functools

import jax
import jax.numpy as jnp
from jax import lax
from jax.experimental import pallas as pl
from jax.experimental.pallas import tpu as pltpu
from jax.sharding import PartitionSpec as P

KEEP_DIV = 8
LANES = 128
QUARTERS = 4
MSG = 16
LOG2E = 1.4426950408889634
NEG = -3e38
SIDE = 4
CHUNKS = 4
BF16 = jnp.bfloat16
F32 = jnp.float32


def layer_norm(hidden):
    hid_f32 = hidden.astype(F32)
    centred = hid_f32 - jnp.mean(hid_f32, axis=-1, keepdims=True)
    row_var = jnp.mean(centred * centred, axis=-1, keepdims=True)
    return (centred * lax.rsqrt(row_var + 1e-6)).astype(BF16)


def gelu(x):
    return 0.5 * x * (1.0 + lax.erf(x * (0.5 ** 0.5)))


def dot(a, b):
    return jnp.dot(a, b, preferred_element_type=F32)


def dot_t(a, b):
    return lax.dot_general(a, b, (((1,), (1,)), ((), ())), preferred_element_type=F32)


def lane_of(shape):
    return lax.broadcasted_iota(jnp.int32, shape, len(shape) - 1)


def roll(x, shift):
    shift = shift % LANES
    return x if shift == 0 else pltpu.roll(x, shift, 1)


def row_of(ref):
    rows = ref[...].astype(F32)
    return jnp.concatenate([rows[i:i + 1] for i in range(rows.shape[0])], axis=1)


def wait_bytes(ref, sem):
    pltpu.make_async_copy(ref, ref, sem).wait()


def model_kernel(n, enc_heads, dec_heads, mask, b_pe, mask_token, patches_h, enc_pos_h, dec_pos_h,
                 w_pe, e_qkv, e_proj, e_up, e_down, w_ed, d_qkv, d_proj, d_up, d_down, w_out, out,
                 patches, enc_pos, dec_pos, w_pe_s, e_qkv_s, e_proj_s, e_up_s, e_down_s, w_ed_s, d_qkv_s, d_proj_s, d_up_s, d_down_s, w_out_s,
                 ekvm, dkvm, qm, o_s, ekv, dkv, q_in, o_in, ekvx, kvt, qq, s_buf, p_buf, hid_e, qkv_e, att_e, hid_d, qkv_d, att_d, pick_s,
                 m_st, l_st, acc_st, wsem, kv_send, kv_recv, f_send, f_recv, q_send, q_recv, o_send, o_recv):
    me = lax.axis_index('sp')
    groups = n // QUARTERS
    pair = me // QUARTERS
    chips = n // 2
    per_chunk = chips // CHUNKS
    core = lax.rem(me, 2)
    partner = me + 1 - 2 * core
    at_z, at_y, at_x = me // 32, lax.rem(me // 8, SIDE), lax.rem(me // 2, SIDE)

    def device_at(dz, dy, dx):
        return (lax.rem(at_z + dz, SIDE) * SIDE + lax.rem(at_y + dy, SIDE)) * 8 + lax.rem(at_x + dx, SIDE) * 2 + core

    far = {0: 0, 1: 1, 2: 2, 3: 1}
    offsets = sorted(((dz, dy, dx) for dz in range(SIDE) for dy in range(SIDE) for dx in range(SIDE)), key=lambda o: far[o[0]] + far[o[1]] + far[o[2]])

    def query_offset(block, j):
        return 2 * lax.rem(block, 2) + j // 4, j % 4, 2 * (block // 2)

    def back(d):
        return SIDE - d
    clips, tokens, _ = patches.shape
    slots = 2 * (tokens // KEEP_DIV)
    layers = e_qkv.shape[0]
    d_enc = enc_pos.shape[1]
    d_dec = dec_pos.shape[1]
    mesh_id = pl.DeviceIdType.MESH

    def load(src, dst, i):
        return pltpu.make_async_copy(src, dst, wsem.at[i])

    load_pe = load(w_pe, w_pe_s, 0)
    load_ed = load(w_ed, w_ed_s, 5)
    load_out = load(w_out, w_out_s, 10)
    enc_loads = [(e_qkv, e_qkv_s, 1), (e_proj, e_proj_s, 2), (e_up, e_up_s, 3), (e_down, e_down_s, 4)]
    dec_loads = [load(d_qkv, d_qkv_s, 6), load(d_proj, d_proj_s, 7), load(d_up, d_up_s, 8), load(d_down, d_down_s, 9)]

    def enc_load(which, layer):
        src, dst, i = enc_loads[which]
        return load(src.at[layer], dst, i)

    first_loads = [load(patches_h, patches, 11), load(enc_pos_h, enc_pos, 12), load(dec_pos_h, dec_pos, 13)]
    for copy in first_loads:
        copy.start()
    load_pe.start()
    enc_load(0, 0).start()

    barrier = pltpu.get_barrier_semaphore()

    def greet(i, _):
        pl.semaphore_signal(barrier, inc=1, device_id={'sp': lax.rem(me + 2 * i, n)}, device_id_type=mesh_id)
        return 0

    lax.fori_loop(1, chips, greet, 0)
    pl.semaphore_signal(barrier, inc=1, device_id={'sp': partner}, device_id_type=mesh_id)

    mask_f = mask[...].astype(F32)
    before = lax.broadcasted_iota(jnp.int32, (tokens, tokens), 0) < lax.broadcasted_iota(jnp.int32, (tokens, tokens), 1)
    rank = dot(mask_f.astype(BF16), before.astype(BF16))
    slot_id = lax.broadcasted_iota(jnp.int32, (slots, tokens), 0).astype(F32)
    selects, moved_x, moved_pos, occupied = [], [], [], []
    for copy in first_loads:
        copy.wait()
    for c in range(clips):
        select = jnp.where((rank[c:c + 1] == slot_id) & (mask_f[c:c + 1] > 0), 1.0, 0.0)
        selects.append(select)
        moved_x.append(dot(select.astype(BF16), patches[c]).astype(BF16))
        moved_pos.append(dot(select.astype(BF16), enc_pos[...]))
        occupied.append(jnp.sum(select, axis=1, keepdims=True))
    load_pe.wait()
    embedded = dot(jnp.concatenate(moved_x, axis=0), w_pe_s[...]) + row_of(b_pe) + jnp.concatenate(moved_pos, axis=0)
    hid_e[...] = embedded.astype(BF16)
    for which in range(1, 4):
        enc_load(which, 0).start()

    def send_kv(phase, kvm, kv, order):
        for i in order:
            to = device_at(*offsets[i])
            pltpu.make_async_remote_copy(
                src_ref=kvm.at[to // QUARTERS], dst_ref=kv.at[i], send_sem=kv_send.at[phase], recv_sem=kv_recv.at[phase, i // per_chunk],
                device_id={'sp': to}, device_id_type=mesh_id).start()

    def send_q(phase, order):
        for k in order:
            to = device_at(*query_offset(k // 8, k % 8))
            pltpu.make_async_remote_copy(
                src_ref=qm.at[to // QUARTERS], dst_ref=q_in.at[phase, k], send_sem=q_send.at[phase], recv_sem=q_recv.at[phase, k // 8],
                device_id={'sp': to}, device_id_type=mesh_id).start()

    def relay(phase, kv, c):
        first = 1 if isinstance(c, int) and c == 0 else 0
        wait_bytes(kv.at[pl.ds(c * per_chunk + first, per_chunk - first)], kv_recv.at[phase, c])
        pltpu.make_async_remote_copy(
            src_ref=kv.at[pl.ds(c * per_chunk, per_chunk)], dst_ref=kv.at[pl.ds(chips + c * per_chunk, per_chunk)],
            send_sem=f_send.at[phase], recv_sem=f_recv.at[phase, c], device_id={'sp': partner}, device_id_type=mesh_id).start()

    def relayed(phase, kv, c):
        wait_bytes(kv.at[pl.ds(chips + c * per_chunk, per_chunk)], f_recv.at[phase, c])

    def queries_in(phase, block):
        first = 1 if isinstance(block, int) and block == 0 else 0
        wait_bytes(q_in.at[phase, pl.ds(8 * block + first, 8 - first)], q_recv.at[phase, block])

    def send_home(phase, block, j):
        dz, dy, dx = query_offset(block, j)
        to = device_at(back(dz), back(dy), back(dx))
        pltpu.make_async_remote_copy(
            src_ref=o_s.at[8 * block + j], dst_ref=o_in.at[phase, pair], send_sem=o_send.at[phase], recv_sem=o_recv.at[phase],
            device_id={'sp': to}, device_id_type=mesh_id).start()

    def finish(phase, kv):
        rest = pl.ds(1, groups - 1)
        wait_bytes(o_in.at[phase, rest], o_recv.at[phase])
        wait_bytes(o_s.at[rest], o_send.at[phase])
        wait_bytes(qm.at[rest], q_send.at[phase])
        wait_bytes(kv.at[pl.ds(1, chips - 1)], kv_send.at[phase])
        wait_bytes(kv.at[pl.ds(0, chips)], f_send.at[phase])

    hd_e = d_enc // enc_heads
    lane_e = lane_of((slots, LANES))
    c_e = hd_e ** -0.5 * LOG2E
    n_e = n * slots
    m_e = groups * slots
    bk = 256

    def enc_layer(layer, _):
        normed = layer_norm(hid_e[...])
        enc_load(0, layer).wait()
        for t in range(d_enc, 3 * d_enc, 1024):
            qkv_e[:, t:t + 1024] = dot_t(normed, e_qkv_s[t:t + 1024])

        for c in range(clips):
            rows = slice(c * slots, (c + 1) * slots)
            for h in range(enc_heads):
                tile = (h * hd_e) // LANES * LANES
                off = h * hd_e - tile
                k_t = roll(qkv_e[rows, d_enc + tile:d_enc + tile + LANES], -off)
                v_t = roll(qkv_e[rows, 2 * d_enc + tile:2 * d_enc + tile + LANES], hd_e - off)
                kv_t = jnp.where(lane_e < hd_e, k_t, v_t)
                ekvm[c * enc_heads + h] = jnp.where(occupied[c] > 0, kv_t, jnp.inf).astype(BF16)

        kv = ekv.at[layer]

        @pl.when(layer == 0)
        def _():
            pl.semaphore_wait(barrier, chips)

        send_kv(layer, ekvm, kv, range(chips - 1, 0, -1))
        qkv_e[:, :d_enc] = dot_t(normed, e_qkv_s[:d_enc])
        for c in range(clips):
            rows = slice(c * slots, (c + 1) * slots)
            for h in range(enc_heads):
                tile = (h * hd_e) // LANES * LANES
                q_t = roll(qkv_e[rows, tile:tile + LANES], tile - h * hd_e)
                qm[c * enc_heads + h] = jnp.where(lane_e < hd_e, q_t, 0.0).astype(BF16)
        send_q(layer, range(groups - 1, 0, -1))
        q_in[layer, 0] = qm[pair]
        kv[0] = ekvm[pair]

        @pl.when(layer + 1 < layers)
        def _():
            enc_load(0, layer + 1).start()

        @pl.when(layer == 0)
        def _():
            load_ed.start()
            for copy in dec_loads:
                copy.start()
            load_out.start()

        for c in (2, 1, 0, 3):
            relay(layer, kv, c)
        for block in range(4):
            queries_in(layer, block)
        for c in (2, 1, 0, 3):
            relayed(layer, kv, c)
        for t in range(0, n, 32):
            block = kv[t:t + 32].reshape(32 * slots, LANES)
            bad = block == jnp.inf
            r = slice(t * slots, (t + 32) * slots)
            clean = jnp.where(bad, jnp.zeros_like(block), block)
            ekvx[r, :LANES] = clean
            ekvx[r, LANES:] = jnp.where(bad & (lane_of(block.shape) == 0), jnp.full_like(block, NEG), jnp.zeros_like(block))
            kvt[:, r] = clean.T
        q = q_in[layer].reshape(m_e, LANES)
        q = jnp.concatenate([q, (lane_of(q.shape) == 0).astype(BF16)], axis=1)
        steps = n_e // bk
        m = jnp.full((1, m_e), NEG, F32)
        l = jnp.zeros((1, m_e), F32)
        acc = jnp.zeros((hd_e, m_e), F32)
        s_buf[0, :, :m_e] = dot_t(ekvx[:bk], q)
        prev = None
        for i in range(steps):
            if i + 1 < steps:
                s_buf[(i + 1) % 2, :, :m_e] = dot_t(ekvx[(i + 1) * bk:(i + 2) * bk], q)
            s = s_buf[i % 2, :, :m_e]
            m_new = jnp.maximum(m, jnp.max(s, axis=0, keepdims=True))
            p = jnp.exp2(s * c_e - m_new * c_e)
            alpha = jnp.exp2((m - m_new) * c_e)
            l = l * alpha + jnp.sum(p, axis=0, keepdims=True)
            p_buf[i % 2, :, :m_e] = p.astype(BF16)
            m = m_new
            if prev is not None:
                j, a = prev
                acc = acc * a + dot(kvt[hd_e:2 * hd_e, j * bk:(j + 1) * bk], p_buf[j % 2, :, :m_e])
            prev = (i, alpha)
        j, a = prev
        acc = acc * a + dot(kvt[hd_e:2 * hd_e, j * bk:(j + 1) * bk], p_buf[j % 2, :, :m_e])
        res = acc / l
        odd = lax.rem(pair, 2) == 1
        zero = jnp.zeros_like(res)
        both = jnp.concatenate([jnp.where(odd, zero, res), jnp.where(odd, res, zero)], axis=0)
        o_s[...] = both.T.astype(BF16).reshape(groups, slots, LANES)

        o_in[layer, pair] = o_s[0]
        for k in range(groups - 1, 0, -1):
            send_home(layer, k // 8, k % 8)
        finish(layer, kv)

        for c in range(clips):
            for g in range(enc_heads // 2):
                first = c * enc_heads + 2 * g
                att_e[c * slots:(c + 1) * slots, g * LANES:(g + 1) * LANES] = (
                    o_in[layer, first].astype(F32) + o_in[layer, first + 1].astype(F32)).astype(BF16)
        enc_load(1, layer).wait()
        mid = (hid_e[...].astype(F32) + dot(att_e[...], e_proj_s[...])).astype(BF16)

        @pl.when(layer + 1 < layers)
        def _():
            enc_load(1, layer + 1).start()

        normed = layer_norm(mid)
        enc_load(2, layer).wait()
        enc_load(3, layer).wait()
        total = mid.astype(F32)
        for t in range(0, e_up_s.shape[1], 1024):
            up = gelu(dot(normed, e_up_s[:, t:t + 1024])).astype(BF16)
            total = total + dot(up, e_down_s[t:t + 1024])

        @pl.when(layer + 1 < layers)
        def _():
            enc_load(2, layer + 1).start()
            enc_load(3, layer + 1).start()

        hid_e[...] = total.astype(BF16)
        return 0

    lax.fori_loop(0, layers, enc_layer, 0)

    load_ed.wait()
    z = dot(layer_norm(hid_e[...]), w_ed_s[...]).astype(BF16)
    for c in range(clips):
        placed = lax.dot_general(selects[c].astype(BF16), z[c * slots:(c + 1) * slots], (((0,), (0,)), ((), ())), preferred_element_type=F32)
        seen = jnp.max(selects[c].T, axis=1, keepdims=True)
        token = jnp.where(seen > 0, placed, row_of(mask_token))
        hid_d[c * tokens:(c + 1) * tokens] = (token + dec_pos[...].astype(F32)).astype(BF16)

    hd_d = d_dec // dec_heads
    c_d = hd_d ** -0.5 * LOG2E
    half = tokens // 2
    parts = LANES // hd_d
    rows_q = tokens // parts
    n_d = n * half
    q_rows = groups * rows_q
    blk = 128
    m_d = 2 * parts * blk
    h_d = m_d // 2
    per = blk // rows_q
    lane_q = lane_of((rows_q, LANES))
    lane_k = lane_of((half, LANES))
    col = lane_of((LANES, 2 * parts * LANES))
    row = lax.broadcasted_iota(jnp.int32, col.shape, 0)
    part = col // LANES
    inside = lax.rem(col, LANES) - jnp.where(part >= parts, 2 * hd_d, 0)
    pick_s[...] = jnp.where((inside >= 0) & (inside < hd_d) & (row == inside + hd_d * lax.rem(part, parts)), 1.0, 0.0).astype(BF16)
    for copy in dec_loads:
        copy.wait()

    def dec_layer(layer, _):
        phase = layers + layer
        normed = layer_norm(hid_d[...])
        kv = dkv.at[layer]
        qkv_d[:, d_dec:] = dot_t(normed, d_qkv_s[layer, d_dec:])
        for c in range(clips):
            base = c * tokens
            for h in range(dec_heads):
                tile = (h * hd_d) // LANES * LANES
                off = h * hd_d - tile
                lo = slice(base, base + half)
                hi = slice(base + half, base + tokens)
                kc = slice(d_dec + tile, d_dec + tile + LANES)
                vc = slice(2 * d_dec + tile, 2 * d_dec + tile + LANES)
                k_lo, v_lo = roll(qkv_d[lo, kc], -off), roll(qkv_d[lo, vc], hd_d - off)
                k_hi, v_hi = roll(qkv_d[hi, kc], 2 * hd_d - off), roll(qkv_d[hi, vc], 3 * hd_d - off)
                dkvm[c * dec_heads + h] = jnp.where(
                    lane_k < 2 * hd_d, jnp.where(lane_k < hd_d, k_lo, v_lo), jnp.where(lane_k < 3 * hd_d, k_hi, v_hi)).astype(BF16)
        send_kv(phase, dkvm, kv, range(1, per_chunk))
        qkv_d[:, :d_dec] = dot_t(normed, d_qkv_s[layer, :d_dec])
        for c in range(clips):
            base = c * tokens
            for h in range(dec_heads):
                tile = (h * hd_d) // LANES * LANES
                off = h * hd_d - tile
                packed = None
                for j in range(parts):
                    moved = roll(qkv_d[base + j * rows_q:base + (j + 1) * rows_q, tile:tile + LANES], hd_d * j - off)
                    packed = moved if packed is None else jnp.where(lane_q >= hd_d * j, moved, packed)
                qm[c * dec_heads + h] = packed.astype(BF16)
        send_q(phase, range(1, groups))
        send_kv(phase, dkvm, kv, range(per_chunk, chips))
        q_in[phase, 0] = qm[pair]
        kv[0] = dkvm[pair]

        msgs = bk // half
        blocks = q_rows // blk

        def spread(block):
            queries_in(phase, block)
            wide = dot(q_in[phase, pl.ds(8 * block, 8)].reshape(blk, LANES), pick_s[...])
            for t in range(2 * parts):
                qq[pl.ds(pl.multiple_of(block * m_d + t * blk, blk), blk)] = wide[:, t * LANES:(t + 1) * LANES].astype(BF16)

        def transpose(places):
            for t in places:
                kvt[:, t * half:t * half + bk] = kv[t:t + msgs].reshape(bk, LANES).T

        def scores(block, message, slot):
            q = qq[pl.ds(pl.multiple_of(block * m_d, m_d), m_d)]
            s_buf[slot] = dot_t(kv[pl.ds(message, msgs)].reshape(bk, LANES), q)

        def attend(block, places, state, next_block, next_message):
            m, l, acc_a, acc_b = state
            alphas = []
            steps = len(places)

            def add(i, acc_a, acc_b):
                keys = slice(places[i] * half, places[i] * half + bk)
                acc_a = acc_a * alphas[i][:, :h_d] + dot(kvt[hd_d:2 * hd_d, keys], p_buf[i % 2, :, :h_d])
                acc_b = acc_b * alphas[i][:, h_d:] + dot(kvt[3 * hd_d:4 * hd_d, keys], p_buf[i % 2, :, h_d:])
                return acc_a, acc_b

            for i in range(steps):
                if i + 1 < steps:
                    scores(block, places[i + 1], (i + 1) % 2)
                else:
                    scores(next_block, next_message, 0)
                s = s_buf[i % 2]
                m_new = jnp.maximum(m, jnp.max(s, axis=0, keepdims=True))
                p = jnp.exp2(s * c_d - m_new * c_d)
                alphas.append(jnp.exp2((m - m_new) * c_d))
                l = l * alphas[i] + jnp.sum(p, axis=0, keepdims=True)
                p_buf[i % 2] = p.astype(BF16)
                m = m_new
                if i > 0:
                    acc_a, acc_b = add(i - 1, acc_a, acc_b)
            acc_a, acc_b = add(steps - 1, acc_a, acc_b)
            return m, l, acc_a, acc_b

        near = [i for i in range(0, per_chunk, msgs)]
        near = near + [chips + i for i in near]

        relay(phase, kv, 0)
        spread(0)
        spread(1)
        relayed(phase, kv, 0)
        transpose(near)
        scores(0, near[0], 0)

        def near_block(b, _):
            @pl.when(b > 0)
            def _():
                relay(phase, kv, b)

            @pl.when(b + 2 < blocks)
            def _():
                spread(b + 2)

            fresh = (jnp.full((1, m_d), NEG, F32), jnp.zeros((1, m_d), F32), jnp.zeros((hd_d, h_d), F32), jnp.zeros((hd_d, h_d), F32))
            state = attend(b, near, fresh, jnp.minimum(b + 1, blocks - 1), b // (blocks - 1) * per_chunk)
            m_st[b], l_st[b], acc_st[b, 0], acc_st[b, 1] = state
            return 0

        lax.fori_loop(0, blocks, near_block, 0)
        for c in range(1, CHUNKS):
            places = [c * per_chunk + i for i in near]
            relayed(phase, kv, c)
            transpose(places)

            def rest_block(b, _):
                block = blocks - 1 - b if c % 2 else b
                if c + 1 == CHUNKS:
                    next_block = jnp.maximum(block - 1, 0)
                elif c % 2:
                    next_block = jnp.maximum(block - 1, 0)
                else:
                    next_block = jnp.minimum(block + 1, blocks - 1)
                ahead = 1 if c + 1 < CHUNKS else 0
                state = (m_st[block], l_st[block], acc_st[block, 0], acc_st[block, 1])
                state = attend(block, places, state, next_block, (c + b // (blocks - 1) * ahead) * per_chunk)
                m, l, acc_a, acc_b = state
                if c + 1 < CHUNKS:
                    m_st[block], l_st[block], acc_st[block, 0], acc_st[block, 1] = state
                    return 0
                m_all = jnp.maximum(m[:, :h_d], m[:, h_d:])
                e_a = jnp.exp2((m[:, :h_d] - m_all) * c_d)
                e_b = jnp.exp2((m[:, h_d:] - m_all) * c_d)
                res = (acc_a * e_a + acc_b * e_b) / (l[:, :h_d] * e_a + l[:, h_d:] * e_b)
                stacked = jnp.concatenate([res[:, j * blk:(j + 1) * blk] for j in range(parts)], axis=0)
                o_s[pl.ds(block * per, per)] = stacked.T.astype(BF16).reshape(per, rows_q, LANES)
                for j in range(1, per):
                    send_home(phase, block, j)

                @pl.when(block > 0)
                def _():
                    send_home(phase, block, 0)
                return 0

            lax.fori_loop(0, blocks, rest_block, 0)
        o_in[phase, pair] = o_s[0]
        finish(phase, kv)

        for c in range(clips):
            for g in range(dec_heads // parts):
                got = [o_in[phase, c * dec_heads + parts * g + h].astype(F32) for h in range(parts)]
                for j in range(parts):
                    tile = None
                    for h in range(parts):
                        moved = roll(got[h], hd_d * (h - j))
                        tile = moved if tile is None else jnp.where(lane_q >= hd_d * h, moved, tile)
                    att_d[c * tokens + j * rows_q:c * tokens + (j + 1) * rows_q, g * LANES:(g + 1) * LANES] = tile.astype(BF16)
        mid = (hid_d[...].astype(F32) + dot(att_d[...], d_proj_s[layer])).astype(BF16)
        up = gelu(dot(layer_norm(mid), d_up_s[layer])).astype(BF16)
        hid_d[...] = (mid.astype(F32) + dot(up, d_down_s[layer])).astype(BF16)
        return 0

    lax.fori_loop(0, layers, dec_layer, 0)
    load_out.wait()
    result = dot(layer_norm(hid_d[...]), w_out_s[...])
    for c in range(clips):
        out[c] = result[c * tokens:(c + 1) * tokens]


def solution(mesh):
    n = mesh.shape['sp']

    def local_program(patches, vis_mask, enc_pos, dec_pos, w_pe, b_pe, enc_qkv, enc_proj, enc_up, enc_down, w_ed, mask_token, dec_qkv, dec_proj, dec_up, dec_down, w_out):
        clips, tokens, width = patches.shape
        layers, d_enc, _, enc_heads, _ = enc_qkv.shape
        _, d_dec, _, dec_heads, _ = dec_qkv.shape
        slots = 2 * (tokens // KEEP_DIV)
        half = tokens // 2
        groups = n // QUARTERS
        f_enc, f_dec = enc_up.shape[2], dec_up.shape[2]
        e_rows, d_rows = clips * slots, clips * tokens
        phases = 2 * layers
        bk, m_d = 256, 1024
        vmem = pl.BlockSpec(memory_space=pltpu.VMEM)
        hbm = pl.BlockSpec(memory_space=pl.ANY)

        def buf(*shape, dtype=BF16):
            return pltpu.VMEM(shape, dtype)

        def sems(*shape):
            return pltpu.SemaphoreType.DMA(shape)

        return pl.pallas_call(
            functools.partial(model_kernel, n, enc_heads, dec_heads),
            out_shape=jax.ShapeDtypeStruct((clips, tokens, w_out.shape[1]), F32),
            in_specs=[vmem] * 3 + [hbm] * 14,
            out_specs=vmem,
            scratch_shapes=[
                buf(clips, tokens, width), buf(tokens, d_enc), buf(tokens, d_dec),
                buf(width, d_enc), buf(3 * d_enc, d_enc), buf(d_enc, d_enc), buf(d_enc, f_enc), buf(f_enc, d_enc), buf(d_enc, d_dec),
                buf(layers, 3 * d_dec, d_dec), buf(layers, d_dec, d_dec), buf(layers, d_dec, f_dec), buf(layers, f_dec, d_dec), buf(d_dec, w_out.shape[1]),
                buf(groups, slots, LANES), buf(groups, half, LANES), buf(groups, MSG, LANES), buf(groups, MSG, LANES),
                buf(layers, n, slots, LANES), buf(layers, n, half, LANES), buf(phases, groups, MSG, LANES), buf(phases, groups, MSG, LANES),
                buf(n * slots, 2 * LANES), buf(LANES, n * half), buf(groups * MSG * 8, LANES),
                buf(2, bk, m_d, dtype=F32), buf(2, bk, m_d),
                buf(e_rows, d_enc), buf(e_rows, 3 * d_enc, dtype=F32), buf(e_rows, d_enc),
                buf(d_rows, d_dec), buf(d_rows, 3 * d_dec, dtype=F32), buf(d_rows, d_dec),
                buf(LANES, 8 * LANES),
                buf(4, 1, m_d, dtype=F32), buf(4, 1, m_d, dtype=F32), buf(4, 2, LANES // 4, m_d // 2, dtype=F32),
                pltpu.SemaphoreType.DMA((14,)),
                sems(phases), sems(phases, CHUNKS), sems(phases), sems(phases, CHUNKS), sems(phases), sems(phases, 4), sems(phases), sems(phases),
            ],
            compiler_params=pltpu.CompilerParams(collective_id=0, has_side_effects=True, vmem_limit_bytes=67043328),
            name='model',
        )(vis_mask, b_pe.reshape(-1, LANES), mask_token.reshape(-1, LANES), patches, enc_pos, dec_pos, w_pe,
          enc_qkv.transpose(0, 2, 3, 4, 1).reshape(layers, 3 * d_enc, d_enc), enc_proj.reshape(layers, d_enc, d_enc), enc_up, enc_down, w_ed,
          dec_qkv.transpose(0, 2, 3, 4, 1).reshape(layers, 3 * d_dec, d_dec), dec_proj.reshape(layers, d_dec, d_dec), dec_up, dec_down, w_out)

    row_spec = P('dp', 'sp', None)
    pos_spec = P(('dp', 'sp'), None)
    arg_specs = (row_spec, P('dp', 'sp'), pos_spec, pos_spec) + (P(),) * 13
    return jax.shard_map(local_program, mesh=mesh, in_specs=arg_specs, out_specs=row_spec, check_vma=False)
```

```python
import functools

import jax
import jax.numpy as jnp
from jax import lax
from jax.experimental import pallas as pl
from jax.experimental.pallas import tpu as pltpu
from jax.sharding import PartitionSpec as P

KEEP_DIV = 8
LANES = 128
QUARTERS = 4
MSG = 16
LOG2E = 1.4426950408889634
NEG = -3e38
SIDE = 4
CHUNKS = 4
BF16 = jnp.bfloat16
F32 = jnp.float32


def layer_norm(hidden):
    hid_f32 = hidden.astype(F32)
    centred = hid_f32 - jnp.mean(hid_f32, axis=-1, keepdims=True)
    row_var = jnp.mean(centred * centred, axis=-1, keepdims=True)
    return (centred * lax.rsqrt(row_var + 1e-6)).astype(BF16)


def gelu(x):
    return 0.5 * x * (1.0 + lax.erf(x * (0.5 ** 0.5)))


def dot(a, b):
    return jnp.dot(a, b, preferred_element_type=F32)


def dot_t(a, b):
    return lax.dot_general(a, b, (((1,), (1,)), ((), ())), preferred_element_type=F32)


def lane_of(shape):
    return lax.broadcasted_iota(jnp.int32, shape, len(shape) - 1)


def roll(x, shift):
    shift = shift % LANES
    return x if shift == 0 else pltpu.roll(x, shift, 1)


def row_of(ref):
    rows = ref[...].astype(F32)
    return jnp.concatenate([rows[i:i + 1] for i in range(rows.shape[0])], axis=1)


def wait_bytes(ref, sem):
    pltpu.make_async_copy(ref, ref, sem).wait()


def model_kernel(n, enc_heads, dec_heads, mask, b_pe, mask_token, patches_h, enc_pos_h, dec_pos_h,
                 w_pe, e_qkv, e_proj, e_up, e_down, w_ed, d_qkv, d_proj, d_up, d_down, w_out, out,
                 patches, enc_pos, dec_pos, w_pe_s, e_qkv_s, e_proj_s, e_up_s, e_down_s, w_ed_s, d_qkv_s, d_proj_s, d_up_s, d_down_s, w_out_s,
                 ekvm, dkvm, eqm, dqm, o_s, ekv, dkv, eq_in, dq_in, o_in, ekvx, kvt, qq, s_buf, p_buf, hid_e, qkv_e, att_e, hid_d, qkv_d, att_d, pick_s,
                 m_st, l_st, acc_st, wsem, kv_send, kv_recv, f_send, f_recv, q_send, q_recv, o_send, o_recv):
    me = lax.axis_index('sp')
    groups = n // QUARTERS
    pair = me // QUARTERS
    chips = n // 2
    per_chunk = chips // CHUNKS
    core = lax.rem(me, 2)
    partner = me + 1 - 2 * core
    at_z, at_y, at_x = me // 32, lax.rem(me // 8, SIDE), lax.rem(me // 2, SIDE)

    def device_at(dz, dy, dx):
        return (lax.rem(at_z + dz, SIDE) * SIDE + lax.rem(at_y + dy, SIDE)) * 8 + lax.rem(at_x + dx, SIDE) * 2 + core

    far = {0: 0, 1: 1, 2: 2, 3: 1}
    offsets = sorted(((dz, dy, dx) for dz in range(SIDE) for dy in range(SIDE) for dx in range(SIDE)), key=lambda o: far[o[0]] + far[o[1]] + far[o[2]])

    def query_offset(block, j):
        return 2 * lax.rem(block, 2) + j // 4, j % 4, 2 * (block // 2)

    def back(d):
        return SIDE - d
    clips, tokens, _ = patches.shape
    slots = 2 * (tokens // KEEP_DIV)
    layers = e_qkv.shape[0]
    d_enc = enc_pos.shape[1]
    d_dec = dec_pos.shape[1]
    mesh_id = pl.DeviceIdType.MESH

    def load(src, dst, i):
        return pltpu.make_async_copy(src, dst, wsem.at[i])

    load_pe = load(w_pe, w_pe_s, 0)
    load_ed = load(w_ed, w_ed_s, 5)
    load_out = load(w_out, w_out_s, 10)
    enc_loads = [(e_qkv, e_qkv_s, 1), (e_proj, e_proj_s, 2), (e_up, e_up_s, 3), (e_down, e_down_s, 4)]
    dec_loads = [load(d_qkv, d_qkv_s, 6), load(d_proj, d_proj_s, 7), load(d_up, d_up_s, 8), load(d_down, d_down_s, 9)]

    def enc_load(which, layer):
        src, dst, i = enc_loads[which]
        return load(src.at[layer], dst, i)

    first_loads = [load(patches_h, patches, 11), load(enc_pos_h, enc_pos, 12), load(dec_pos_h, dec_pos, 13)]
    for copy in first_loads:
        copy.start()
    load_pe.start()
    enc_load(0, 0).start()

    barrier = pltpu.get_barrier_semaphore()

    def greet(i, _):
        pl.semaphore_signal(barrier, inc=1, device_id={'sp': lax.rem(me + 2 * i, n)}, device_id_type=mesh_id)
        return 0

    lax.fori_loop(1, chips, greet, 0)
    pl.semaphore_signal(barrier, inc=1, device_id={'sp': partner}, device_id_type=mesh_id)

    mask_f = mask[...].astype(F32)
    before = lax.broadcasted_iota(jnp.int32, (tokens, tokens), 0) < lax.broadcasted_iota(jnp.int32, (tokens, tokens), 1)
    rank = dot(mask_f.astype(BF16), before.astype(BF16))
    slot_id = lax.broadcasted_iota(jnp.int32, (slots, tokens), 0).astype(F32)
    selects, moved_x, moved_pos, occupied = [], [], [], []
    for copy in first_loads:
        copy.wait()
    for c in range(clips):
        select = jnp.where((rank[c:c + 1] == slot_id) & (mask_f[c:c + 1] > 0), 1.0, 0.0)
        selects.append(select)
        moved_x.append(dot(select.astype(BF16), patches[c]).astype(BF16))
        moved_pos.append(dot(select.astype(BF16), enc_pos[...]))
        occupied.append(jnp.sum(select, axis=1, keepdims=True))
    load_pe.wait()
    embedded = dot(jnp.concatenate(moved_x, axis=0), w_pe_s[...]) + row_of(b_pe) + jnp.concatenate(moved_pos, axis=0)
    hid_e[...] = embedded.astype(BF16)
    for which in range(1, 4):
        enc_load(which, 0).start()

    def send_kv(phase, kvm, kv, order):
        for i in order:
            to = device_at(*offsets[i])
            pltpu.make_async_remote_copy(
                src_ref=kvm.at[to // QUARTERS], dst_ref=kv.at[i], send_sem=kv_send.at[phase], recv_sem=kv_recv.at[phase, i // per_chunk],
                device_id={'sp': to}, device_id_type=mesh_id).start()

    def send_q(phase, qm, q_in, order):
        for k in order:
            to = device_at(*query_offset(k // 8, k % 8))
            pltpu.make_async_remote_copy(
                src_ref=qm.at[to // QUARTERS], dst_ref=q_in.at[k], send_sem=q_send.at[phase], recv_sem=q_recv.at[phase, k // 8],
                device_id={'sp': to}, device_id_type=mesh_id).start()

    def relay(phase, kv, c):
        first = 1 if isinstance(c, int) and c == 0 else 0
        wait_bytes(kv.at[pl.ds(c * per_chunk + first, per_chunk - first)], kv_recv.at[phase, c])
        pltpu.make_async_remote_copy(
            src_ref=kv.at[pl.ds(c * per_chunk, per_chunk)], dst_ref=kv.at[pl.ds(chips + c * per_chunk, per_chunk)],
            send_sem=f_send.at[phase], recv_sem=f_recv.at[phase, c], device_id={'sp': partner}, device_id_type=mesh_id).start()

    def relayed(phase, kv, c):
        wait_bytes(kv.at[pl.ds(chips + c * per_chunk, per_chunk)], f_recv.at[phase, c])

    def queries_in(phase, q_in, block):
        first = 1 if isinstance(block, int) and block == 0 else 0
        wait_bytes(q_in.at[pl.ds(8 * block + first, 8 - first)], q_recv.at[phase, block])

    def send_home(phase, block, j):
        dz, dy, dx = query_offset(block, j)
        to = device_at(back(dz), back(dy), back(dx))
        pltpu.make_async_remote_copy(
            src_ref=o_s.at[8 * block + j], dst_ref=o_in.at[phase, pair], send_sem=o_send.at[phase], recv_sem=o_recv.at[phase],
            device_id={'sp': to}, device_id_type=mesh_id).start()

    def finish(phase, kv, qm):
        rest = pl.ds(1, groups - 1)
        wait_bytes(o_in.at[phase, rest], o_recv.at[phase])
        wait_bytes(o_s.at[rest], o_send.at[phase])
        wait_bytes(qm.at[rest], q_send.at[phase])
        wait_bytes(kv.at[pl.ds(1, chips - 1)], kv_send.at[phase])
        wait_bytes(kv.at[pl.ds(0, chips)], f_send.at[phase])

    hd_e = d_enc // enc_heads
    lane_e = lane_of((slots, LANES))
    c_e = hd_e ** -0.5 * LOG2E
    n_e = n * slots
    m_e = groups * slots
    bk = 256

    def enc_layer(layer, _):
        normed = layer_norm(hid_e[...])
        enc_load(0, layer).wait()
        for t in range(d_enc, 3 * d_enc, 1024):
            qkv_e[:, t:t + 1024] = dot_t(normed, e_qkv_s[t:t + 1024])

        for c in range(clips):
            rows = slice(c * slots, (c + 1) * slots)
            for h in range(enc_heads):
                tile = (h * hd_e) // LANES * LANES
                off = h * hd_e - tile
                k_t = roll(qkv_e[rows, d_enc + tile:d_enc + tile + LANES], -off)
                v_t = roll(qkv_e[rows, 2 * d_enc + tile:2 * d_enc + tile + LANES], hd_e - off)
                kv_t = jnp.where(lane_e < hd_e, k_t, v_t)
                ekvm[c * enc_heads + h] = jnp.where(occupied[c] > 0, kv_t, jnp.inf).astype(BF16)

        kv = ekv.at[layer]

        @pl.when(layer == 0)
        def _():
            pl.semaphore_wait(barrier, chips)

        send_kv(layer, ekvm, kv, range(chips - 1, 0, -1))
        qkv_e[:, :d_enc] = dot_t(normed, e_qkv_s[:d_enc])
        for c in range(clips):
            rows = slice(c * slots, (c + 1) * slots)
            for h in range(enc_heads):
                tile = (h * hd_e) // LANES * LANES
                q_t = roll(qkv_e[rows, tile:tile + LANES], tile - h * hd_e)
                low = slots // 2
                eqm[c * enc_heads + h] = jnp.where(lane_of((low, LANES)) < hd_e, q_t[:low], roll(q_t[low:], hd_e)).astype(BF16)
        eq = eq_in.at[layer]
        send_q(layer, eqm, eq, range(groups - 1, 0, -1))
        eq[0] = eqm[pair]
        kv[0] = ekvm[pair]

        @pl.when(layer + 1 < layers)
        def _():
            enc_load(0, layer + 1).start()

        @pl.when(layer == 0)
        def _():
            load_ed.start()
            for copy in dec_loads:
                copy.start()
            load_out.start()

        for c in (2, 1, 0, 3):
            relay(layer, kv, c)
        for block in range(4):
            queries_in(layer, eq, block)
        for c in (2, 1, 0, 3):
            relayed(layer, kv, c)
        for t in range(0, n, 32):
            block = kv[t:t + 32].reshape(32 * slots, LANES)
            bad = block == jnp.inf
            r = slice(t * slots, (t + 32) * slots)
            clean = jnp.where(bad, jnp.zeros_like(block), block)
            ekvx[r, :LANES] = clean
            ekvx[r, LANES:] = jnp.where(bad & (lane_of(block.shape) == 0), jnp.full_like(block, NEG), jnp.zeros_like(block))
            kvt[:, r] = clean.T
        q = eq[...].astype(F32).reshape(m_e // 2, LANES)
        own = lane_of(q.shape) < hd_e
        q = jnp.concatenate([jnp.where(own, q, 0.0), jnp.where(own, roll(q, hd_e), 0.0)], axis=0).astype(BF16)
        q = jnp.concatenate([q, (lane_of(q.shape) == 0).astype(BF16)], axis=1)
        steps = n_e // bk
        m = jnp.full((1, m_e), NEG, F32)
        l = jnp.zeros((1, m_e), F32)
        acc = jnp.zeros((hd_e, m_e), F32)
        s_buf[0, :, :m_e] = dot_t(ekvx[:bk], q)
        prev = None
        for i in range(steps):
            if i + 1 < steps:
                s_buf[(i + 1) % 2, :, :m_e] = dot_t(ekvx[(i + 1) * bk:(i + 2) * bk], q)
            s = s_buf[i % 2, :, :m_e]
            m_new = jnp.maximum(m, jnp.max(s, axis=0, keepdims=True))
            p = jnp.exp2(s * c_e - m_new * c_e)
            alpha = jnp.exp2((m - m_new) * c_e)
            l = l * alpha + jnp.sum(p, axis=0, keepdims=True)
            p_buf[i % 2, :, :m_e] = p.astype(BF16)
            m = m_new
            if prev is not None:
                j, a = prev
                acc = acc * a + dot(kvt[hd_e:2 * hd_e, j * bk:(j + 1) * bk], p_buf[j % 2, :, :m_e])
            prev = (i, alpha)
        j, a = prev
        acc = acc * a + dot(kvt[hd_e:2 * hd_e, j * bk:(j + 1) * bk], p_buf[j % 2, :, :m_e])
        res = acc / l
        odd = lax.rem(pair, 2) == 1
        zero = jnp.zeros_like(res)
        both = jnp.concatenate([jnp.where(odd, zero, res), jnp.where(odd, res, zero)], axis=0)
        both = both.T
        low = slots // 2
        o_s[...] = jnp.concatenate([
            both[:m_e // 2].reshape(groups, low, LANES), both[m_e // 2:].reshape(groups, low, LANES)], axis=1).astype(BF16)

        o_in[layer, pair] = o_s[0]
        for k in range(groups - 1, 0, -1):
            send_home(layer, k // 8, k % 8)
        finish(layer, kv, eqm)

        for c in range(clips):
            for g in range(enc_heads // 2):
                first = c * enc_heads + 2 * g
                att_e[c * slots:(c + 1) * slots, g * LANES:(g + 1) * LANES] = (
                    o_in[layer, first].astype(F32) + o_in[layer, first + 1].astype(F32)).astype(BF16)
        enc_load(1, layer).wait()
        mid = (hid_e[...].astype(F32) + dot(att_e[...], e_proj_s[...])).astype(BF16)

        @pl.when(layer + 1 < layers)
        def _():
            enc_load(1, layer + 1).start()

        normed = layer_norm(mid)
        enc_load(2, layer).wait()
        enc_load(3, layer).wait()
        total = mid.astype(F32)
        for t in range(0, e_up_s.shape[1], 1024):
            up = gelu(dot(normed, e_up_s[:, t:t + 1024])).astype(BF16)
            total = total + dot(up, e_down_s[t:t + 1024])

        @pl.when(layer + 1 < layers)
        def _():
            enc_load(2, layer + 1).start()
            enc_load(3, layer + 1).start()

        hid_e[...] = total.astype(BF16)
        return 0

    lax.fori_loop(0, layers, enc_layer, 0)

    load_ed.wait()
    z = dot(layer_norm(hid_e[...]), w_ed_s[...]).astype(BF16)
    for c in range(clips):
        placed = lax.dot_general(selects[c].astype(BF16), z[c * slots:(c + 1) * slots], (((0,), (0,)), ((), ())), preferred_element_type=F32)
        seen = jnp.max(selects[c].T, axis=1, keepdims=True)
        token = jnp.where(seen > 0, placed, row_of(mask_token))
        hid_d[c * tokens:(c + 1) * tokens] = (token + dec_pos[...].astype(F32)).astype(BF16)

    hd_d = d_dec // dec_heads
    c_d = hd_d ** -0.5 * LOG2E
    half = tokens // 2
    parts = LANES // hd_d
    rows_q = tokens // parts
    n_d = n * half
    q_rows = groups * rows_q
    blk = 128
    m_d = 2 * parts * blk
    h_d = m_d // 2
    per = blk // rows_q
    lane_q = lane_of((rows_q, LANES))
    lane_k = lane_of((half, LANES))
    col = lane_of((LANES, 2 * parts * LANES))
    row = lax.broadcasted_iota(jnp.int32, col.shape, 0)
    part = col // LANES
    inside = lax.rem(col, LANES) - jnp.where(part >= parts, 2 * hd_d, 0)
    pick_s[...] = jnp.where((inside >= 0) & (inside < hd_d) & (row == inside + hd_d * lax.rem(part, parts)), 1.0, 0.0).astype(BF16)
    for copy in dec_loads:
        copy.wait()

    def dec_layer(layer, _):
        phase = layers + layer
        normed = layer_norm(hid_d[...])
        kv = dkv.at[layer]
        qkv_d[:, d_dec:] = dot_t(normed, d_qkv_s[layer, d_dec:])
        for c in range(clips):
            base = c * tokens
            for h in range(dec_heads):
                tile = (h * hd_d) // LANES * LANES
                off = h * hd_d - tile
                lo = slice(base, base + half)
                hi = slice(base + half, base + tokens)
                kc = slice(d_dec + tile, d_dec + tile + LANES)
                vc = slice(2 * d_dec + tile, 2 * d_dec + tile + LANES)
                k_lo, v_lo = roll(qkv_d[lo, kc], -off), roll(qkv_d[lo, vc], hd_d - off)
                k_hi, v_hi = roll(qkv_d[hi, kc], 2 * hd_d - off), roll(qkv_d[hi, vc], 3 * hd_d - off)
                dkvm[c * dec_heads + h] = jnp.where(
                    lane_k < 2 * hd_d, jnp.where(lane_k < hd_d, k_lo, v_lo), jnp.where(lane_k < 3 * hd_d, k_hi, v_hi)).astype(BF16)
        send_kv(phase, dkvm, kv, range(1, per_chunk))
        qkv_d[:, :d_dec] = dot_t(normed, d_qkv_s[layer, :d_dec])
        for c in range(clips):
            base = c * tokens
            for h in range(dec_heads):
                tile = (h * hd_d) // LANES * LANES
                off = h * hd_d - tile
                packed = None
                for j in range(parts):
                    moved = roll(qkv_d[base + j * rows_q:base + (j + 1) * rows_q, tile:tile + LANES], hd_d * j - off)
                    packed = moved if packed is None else jnp.where(lane_q >= hd_d * j, moved, packed)
                dqm[c * dec_heads + h] = packed.astype(BF16)
        dq = dq_in.at[layer]
        send_q(phase, dqm, dq, range(1, groups))
        send_kv(phase, dkvm, kv, range(per_chunk, chips))
        dq[0] = dqm[pair]
        kv[0] = dkvm[pair]

        msgs = bk // half
        blocks = q_rows // blk

        def spread(block):
            queries_in(phase, dq, block)
            wide = dot(dq[pl.ds(8 * block, 8)].reshape(blk, LANES), pick_s[...])
            for t in range(2 * parts):
                qq[pl.ds(pl.multiple_of(block * m_d + t * blk, blk), blk)] = wide[:, t * LANES:(t + 1) * LANES].astype(BF16)

        def transpose(places):
            for t in places:
                kvt[:, t * half:t * half + bk] = kv[t:t + msgs].reshape(bk, LANES).T

        def scores(block, message, slot):
            q = qq[pl.ds(pl.multiple_of(block * m_d, m_d), m_d)]
            s_buf[slot] = dot_t(kv[pl.ds(message, msgs)].reshape(bk, LANES), q)

        def attend(block, places, state, next_block, next_message):
            m, l, acc_a, acc_b = state
            alphas = []
            steps = len(places)

            def add(i, acc_a, acc_b):
                keys = slice(places[i] * half, places[i] * half + bk)
                acc_a = acc_a * alphas[i][:, :h_d] + dot(kvt[hd_d:2 * hd_d, keys], p_buf[i % 2, :, :h_d])
                acc_b = acc_b * alphas[i][:, h_d:] + dot(kvt[3 * hd_d:4 * hd_d, keys], p_buf[i % 2, :, h_d:])
                return acc_a, acc_b

            for i in range(steps):
                if i + 1 < steps:
                    scores(block, places[i + 1], (i + 1) % 2)
                else:
                    scores(next_block, next_message, 0)
                s = s_buf[i % 2]
                m_new = jnp.maximum(m, jnp.max(s, axis=0, keepdims=True))
                p = jnp.exp2(s * c_d - m_new * c_d)
                alphas.append(jnp.exp2((m - m_new) * c_d))
                l = l * alphas[i] + jnp.sum(p, axis=0, keepdims=True)
                p_buf[i % 2] = p.astype(BF16)
                m = m_new
                if i > 0:
                    acc_a, acc_b = add(i - 1, acc_a, acc_b)
            acc_a, acc_b = add(steps - 1, acc_a, acc_b)
            return m, l, acc_a, acc_b

        near = [i for i in range(0, per_chunk, msgs)]
        near = near + [chips + i for i in near]

        relay(phase, kv, 0)
        spread(0)
        spread(1)
        relayed(phase, kv, 0)
        transpose(near)
        scores(0, near[0], 0)

        def near_block(b, _):
            @pl.when(b > 0)
            def _():
                relay(phase, kv, b)

            @pl.when(b + 2 < blocks)
            def _():
                spread(b + 2)

            fresh = (jnp.full((1, m_d), NEG, F32), jnp.zeros((1, m_d), F32), jnp.zeros((hd_d, h_d), F32), jnp.zeros((hd_d, h_d), F32))
            state = attend(b, near, fresh, jnp.minimum(b + 1, blocks - 1), b // (blocks - 1) * per_chunk)
            m_st[b], l_st[b], acc_st[b, 0], acc_st[b, 1] = state
            return 0

        lax.fori_loop(0, blocks, near_block, 0)
        for c in range(1, CHUNKS):
            places = [c * per_chunk + i for i in near]
            relayed(phase, kv, c)
            transpose(places)

            def rest_block(b, _):
                block = blocks - 1 - b if c % 2 else b
                if c + 1 == CHUNKS:
                    next_block = jnp.maximum(block - 1, 0)
                elif c % 2:
                    next_block = jnp.maximum(block - 1, 0)
                else:
                    next_block = jnp.minimum(block + 1, blocks - 1)
                ahead = 1 if c + 1 < CHUNKS else 0
                state = (m_st[block], l_st[block], acc_st[block, 0], acc_st[block, 1])
                state = attend(block, places, state, next_block, (c + b // (blocks - 1) * ahead) * per_chunk)
                m, l, acc_a, acc_b = state
                if c + 1 < CHUNKS:
                    m_st[block], l_st[block], acc_st[block, 0], acc_st[block, 1] = state
                    return 0
                m_all = jnp.maximum(m[:, :h_d], m[:, h_d:])
                e_a = jnp.exp2((m[:, :h_d] - m_all) * c_d)
                e_b = jnp.exp2((m[:, h_d:] - m_all) * c_d)
                res = (acc_a * e_a + acc_b * e_b) / (l[:, :h_d] * e_a + l[:, h_d:] * e_b)
                stacked = jnp.concatenate([res[:, j * blk:(j + 1) * blk] for j in range(parts)], axis=0)
                o_s[pl.ds(block * per, per)] = stacked.T.astype(BF16).reshape(per, rows_q, LANES)
                for j in range(1, per):
                    send_home(phase, block, j)

                @pl.when(block > 0)
                def _():
                    send_home(phase, block, 0)
                return 0

            lax.fori_loop(0, blocks, rest_block, 0)
        o_in[phase, pair] = o_s[0]
        finish(phase, kv, dqm)

        for c in range(clips):
            for g in range(dec_heads // parts):
                got = [o_in[phase, c * dec_heads + parts * g + h].astype(F32) for h in range(parts)]
                for j in range(parts):
                    tile = None
                    for h in range(parts):
                        moved = roll(got[h], hd_d * (h - j))
                        tile = moved if tile is None else jnp.where(lane_q >= hd_d * h, moved, tile)
                    att_d[c * tokens + j * rows_q:c * tokens + (j + 1) * rows_q, g * LANES:(g + 1) * LANES] = tile.astype(BF16)
        mid = (hid_d[...].astype(F32) + dot(att_d[...], d_proj_s[layer])).astype(BF16)
        up = gelu(dot(layer_norm(mid), d_up_s[layer])).astype(BF16)
        hid_d[...] = (mid.astype(F32) + dot(up, d_down_s[layer])).astype(BF16)
        return 0

    lax.fori_loop(0, layers, dec_layer, 0)
    load_out.wait()
    result = dot(layer_norm(hid_d[...]), w_out_s[...])
    for c in range(clips):
        out[c] = result[c * tokens:(c + 1) * tokens]


def solution(mesh):
    n = mesh.shape['sp']

    def local_program(patches, vis_mask, enc_pos, dec_pos, w_pe, b_pe, enc_qkv, enc_proj, enc_up, enc_down, w_ed, mask_token, dec_qkv, dec_proj, dec_up, dec_down, w_out):
        clips, tokens, width = patches.shape
        layers, d_enc, _, enc_heads, _ = enc_qkv.shape
        _, d_dec, _, dec_heads, _ = dec_qkv.shape
        slots = 2 * (tokens // KEEP_DIV)
        half = tokens // 2
        groups = n // QUARTERS
        f_enc, f_dec = enc_up.shape[2], dec_up.shape[2]
        e_rows, d_rows = clips * slots, clips * tokens
        phases = 2 * layers
        bk, m_d = 256, 1024
        vmem = pl.BlockSpec(memory_space=pltpu.VMEM)
        hbm = pl.BlockSpec(memory_space=pl.ANY)

        def buf(*shape, dtype=BF16):
            return pltpu.VMEM(shape, dtype)

        def sems(*shape):
            return pltpu.SemaphoreType.DMA(shape)

        return pl.pallas_call(
            functools.partial(model_kernel, n, enc_heads, dec_heads),
            out_shape=jax.ShapeDtypeStruct((clips, tokens, w_out.shape[1]), F32),
            in_specs=[vmem] * 3 + [hbm] * 14,
            out_specs=vmem,
            scratch_shapes=[
                buf(clips, tokens, width), buf(tokens, d_enc), buf(tokens, d_dec),
                buf(width, d_enc), buf(3 * d_enc, d_enc), buf(d_enc, d_enc), buf(d_enc, f_enc), buf(f_enc, d_enc), buf(d_enc, d_dec),
                buf(layers, 3 * d_dec, d_dec), buf(layers, d_dec, d_dec), buf(layers, d_dec, f_dec), buf(layers, f_dec, d_dec), buf(d_dec, w_out.shape[1]),
                buf(groups, slots, LANES), buf(groups, half, LANES), buf(groups, slots // 2, LANES), buf(groups, MSG, LANES), buf(groups, MSG, LANES),
                buf(layers, n, slots, LANES), buf(layers, n, half, LANES), buf(layers, groups, slots // 2, LANES), buf(layers, groups, MSG, LANES), buf(phases, groups, MSG, LANES),
                buf(n * slots, 2 * LANES), buf(LANES, n * half), buf(groups * MSG * 8, LANES),
                buf(2, bk, m_d, dtype=F32), buf(2, bk, m_d),
                buf(e_rows, d_enc), buf(e_rows, 3 * d_enc, dtype=F32), buf(e_rows, d_enc),
                buf(d_rows, d_dec), buf(d_rows, 3 * d_dec, dtype=F32), buf(d_rows, d_dec),
                buf(LANES, 8 * LANES),
                buf(4, 1, m_d, dtype=F32), buf(4, 1, m_d, dtype=F32), buf(4, 2, LANES // 4, m_d // 2, dtype=F32),
                pltpu.SemaphoreType.DMA((14,)),
                sems(phases), sems(phases, CHUNKS), sems(phases), sems(phases, CHUNKS), sems(phases), sems(phases, 4), sems(phases), sems(phases),
            ],
            compiler_params=pltpu.CompilerParams(collective_id=0, has_side_effects=True, vmem_limit_bytes=67043328),
            name='model',
        )(vis_mask, b_pe.reshape(-1, LANES), mask_token.reshape(-1, LANES), patches, enc_pos, dec_pos, w_pe,
          enc_qkv.transpose(0, 2, 3, 4, 1).reshape(layers, 3 * d_enc, d_enc), enc_proj.reshape(layers, d_enc, d_enc), enc_up, enc_down, w_ed,
          dec_qkv.transpose(0, 2, 3, 4, 1).reshape(layers, 3 * d_dec, d_dec), dec_proj.reshape(layers, d_dec, d_dec), dec_up, dec_down, w_out)

    row_spec = P('dp', 'sp', None)
    pos_spec = P(('dp', 'sp'), None)
    arg_specs = (row_spec, P('dp', 'sp'), pos_spec, pos_spec) + (P(),) * 13
    return jax.shard_map(local_program, mesh=mesh, in_specs=arg_specs, out_specs=row_spec, check_vma=False)
```
